256 devices in a mesh: row: 8 (over y, z_lo), col: 8 (over z_hi, core), layer: 4 (over x).
Axes of the slice: x: 4, y: 4, z: 8 (z_hi: 4, z_lo: 2; z = z_hi * 2 + z_lo), core: 2. Of those that a mesh axis runs over, the one named last changes fastest.
Arguments:
- density_tiles: bfloat16 [192, 8, 2, 128, 128], P(('row', 'col')), may hold values from -1.5 to 1.5
- tile_columns: int32 [192, 8, 2], P(('row', 'col')), may hold values from -1 to 191, as said below
Outputs:
- square_tiles: bfloat16 [192, 8, 2, 128, 128], P(('row', 'col'), None, None, 'layer')
The draws below stay inside these ranges and needn't reach their ends.
Inputs may be any that keep to these rules, and one draw needn't show every extreme that they name: `tile_columns`: entry [i, g, s] is a tile column in group g (columns g * 24 to (g + 1) * 24 - 1) or -1; within one block row and group the listed columns are distinct and empty slots come after the listed ones; block row i lists its own column i in the first slot of its group, whose 2 slots are all listed; other groups hold 0 to 2 listed tiles.
All inputs are finite; a program needn't handle non-finite values.
Results may differ from the reference program's by a relative error of at most 0.0048.
Values may be sent and summed in bfloat16 or wider, within the bound.
No kernel may reach another device: no remote copies, remote signals or barrier semaphores. Data moves between devices by JAX's collectives and lax.ppermute only.
A program may use at most 64 MiB of HBM per device.

```python
import jax
import jax.numpy as jnp
from jax import lax

TB = 128
NB = 192
KG = 2
NGROUP = 8
GWIDTH = 24
N_LAYER = 4


def draw_tile_columns(key, part):
    shuffle_key, anchor_key, count_key = jax.random.split(jax.random.fold_in(key, 17), 3)
    row_index = jnp.arange(NB, dtype=jnp.int32)
    group_index = jnp.arange(NGROUP, dtype=jnp.int32)

    def shuffled(sub_key):
        return jax.random.permutation(sub_key, GWIDTH - 1)[:KG - 1].astype(jnp.int32)
    offsets = jax.vmap(shuffled)(jax.random.split(shuffle_key, NB * NGROUP)).reshape(NB, NGROUP, KG - 1)
    anchors = jax.random.randint(anchor_key, (NB, NGROUP), 0, GWIDTH).astype(jnp.int32)
    own_group = row_index // GWIDTH
    is_own = own_group[:, None] == group_index[None, :]
    anchors = jnp.where(is_own, (row_index % GWIDTH)[:, None], anchors)
    local_column = jnp.concatenate([anchors[:, :, None], (anchors[:, :, None] + 1 + offsets) % GWIDTH], axis=-1)
    apart = jnp.abs(group_index[None, :] - own_group[:, None])
    distance = jnp.minimum(apart, NGROUP - apart)
    drawn_count = jax.random.randint(count_key, (NB, NGROUP), 0, KG + 1).astype(jnp.int32)
    live_count = jnp.where(distance <= 1, KG, drawn_count)
    slot_index = jnp.arange(KG, dtype=jnp.int32)
    columns = local_column + group_index[None, :, None] * GWIDTH
    return jnp.where(slot_index[None, None, :] < live_count[:, :, None], columns, -1).astype(jnp.int32)


def block_scale(own_key, dims, shards, smallest, high):
    factor_of = 1.0
    for axis_at, parts in shards:
        steps = jax.random.uniform(jax.random.fold_in(jax.random.fold_in(own_key, 6), axis_at), (parts,), jnp.float32, smallest / len(shards), high / len(shards))
        factor_of = factor_of * jnp.repeat(jnp.exp(steps), dims[axis_at] // parts).reshape((-1,) + (1,) * (len(dims) - 1 - axis_at))
    return factor_of


def gaussian(key, extent, width, most, cuts=(), kind=jnp.bfloat16):
    gain = block_scale(key, extent, cuts, -0.22, 0.18) if cuts else 1.0
    result = jax.random.normal(key, extent, jnp.float32) * width * gain
    return jnp.minimum(jnp.maximum(result, -most), most).astype(kind)


def setup_inputs(seed: int = 0) -> dict:
    key_list = jax.random.split(jax.random.key(seed), 3)
    density_tiles = gaussian(key_list[0], (NB, NGROUP, KG, TB, TB), 0.25, 1.5, ((0, 64),))
    tile_columns = draw_tile_columns(jax.random.fold_in(key_list[2], 71), 0)
    return dict(density_tiles=density_tiles, tile_columns=tile_columns)


def reference(density_tiles, tile_columns):
    block_count, group_count, group_slots, tile_side, _ = density_tiles.shape
    row_width = group_count * group_slots
    per_layer = group_count // N_LAYER
    flat_tiles = density_tiles.reshape(block_count, row_width, tile_side, tile_side)
    flat_columns = tile_columns.reshape(block_count, row_width)

    def one_row(row_index):
        own_columns = flat_columns[row_index]
        own_tiles = flat_tiles[row_index]
        is_live = own_columns >= 0
        inner_rows = jnp.where(is_live, own_columns, 0).astype(jnp.int32)
        inner_columns = flat_columns[inner_rows]
        matches = (inner_columns[:, None, :] == own_columns[None, :, None]) & is_live[:, None, None] & is_live[None, :, None]
        slot_index = jnp.argmax(matches.astype(jnp.int32), axis=-1).astype(jnp.int32)
        located = jnp.any(matches, axis=-1)
        selected = flat_tiles[inner_rows[:, None], slot_index].astype(jnp.float32)
        selected = jnp.where(located[:, :, None, None], selected, jnp.float32(0.0))
        left_tiles = own_tiles.astype(jnp.float32).reshape(N_LAYER, per_layer * group_slots, tile_side, tile_side)
        selected = selected.reshape(N_LAYER, per_layer * group_slots, row_width, tile_side, tile_side)
        partial_value = jnp.einsum("larc,lascd->lsrd", left_tiles, selected)
        rounded = lax.optimization_barrier(partial_value.astype(jnp.bfloat16))
        layer_total = jnp.sum(rounded.astype(jnp.float32), axis=0)
        return layer_total.astype(jnp.bfloat16).reshape(group_count, group_slots, tile_side, tile_side)

    return lax.map(one_row, jnp.arange(block_count, dtype=jnp.int32))
```

```python
import functools

import jax
import jax.numpy as jnp
from jax import lax
from jax.experimental import pallas as pl
from jax.experimental.pallas import tpu as pltpu
from jax.sharding import Mesh
from jax.sharding import PartitionSpec as P


ROWS_COLS = ("y", "z_lo", "z_hi", "core")
Z = ("z_lo", "z_hi")
ZC = ("z_lo", "z_hi", "core")
TAIL = 16
EMPTY_TARGET = -3


def z_place(z, n_hi, n_lo):
    z = z % (n_hi * n_lo)
    return (z % n_lo) * n_hi + z // n_lo


def z_steps(step, flip, n_hi, n_lo):
    n = n_hi * n_lo
    return [
        (z_place(z, n_hi, n_lo) * 2 + c, z_place(z + step, n_hi, n_lo) * 2 + (c ^ flip))
        for z in range(n)
        for c in range(2)
    ]


def with_tail(tiles, tail_rows):
    tail = jnp.pad(tail_rows, ((0, TAIL - tail_rows.shape[0]), (0, 128 - tail_rows.shape[1])))
    return jnp.concatenate([tiles.reshape(-1, tiles.shape[-1]), tail.astype(tiles.dtype)], axis=0)


def products(n_left, n_right, rows, slots, left_index, targets, places, *refs):
    tb = 128
    left_in = refs[:n_left]
    right_in = refs[n_left : n_left + n_right]
    out, left, right, right_columns, left_sem, right_sem = refs[n_left + n_right :]
    for n, ref in enumerate(left_in):
        pltpu.make_async_copy(ref, left.at[n], left_sem.at[n]).start()
    for n, ref in enumerate(right_in):
        pltpu.make_async_copy(ref, right.at[n], right_sem.at[n]).start()
    for n, ref in enumerate(right_in):
        pltpu.make_async_copy(ref, right.at[n], right_sem.at[n]).wait()
        right_columns[pl.ds(n * TAIL, TAIL), :] = right[n, pl.ds(rows * slots * tb, TAIL), :].astype(
            jnp.float32
        )
    for n, ref in enumerate(left_in):
        pltpu.make_async_copy(ref, left.at[n], left_sem.at[n]).wait()

    terms = 2 * slots

    def one_source(n, carry):
        place = places[n]
        for row in range(rows):
            i = n * rows + row
            total = jnp.zeros((tb, slots * tb), jnp.float32)
            for first in range(0, terms, 2):
                lefts, rights = [], []
                for term in (first, first + 1):
                    lefts.append(left[n, pl.ds((row * terms + term) * tb, tb), :])
                    inner = left_index[i * terms + term]
                    source = inner // rows
                    inner_row = inner - source * rows
                    tiles = [
                        right[
                            source,
                            pl.ds(pl.multiple_of((inner_row * slots + slot) * tb, tb), tb),
                            :,
                        ]
                        for slot in range(slots)
                    ]
                    columns = [
                        right_columns[pl.ds(source * TAIL + inner_row * slots + slot, 1), :]
                        for slot in range(slots)
                    ]
                    live = (left_index[rows * n_left * terms + i * terms + term]).astype(jnp.float32)
                    wanted = []
                    for target in range(slots):
                        number = targets[i * slots + target].astype(jnp.float32)
                        picked = None
                        for slot in range(slots):
                            match = jnp.where(columns[slot] == number, live, 0.0).astype(jnp.bfloat16)
                            part = tiles[slot] * match
                            picked = part if picked is None else picked + part
                        wanted.append(picked)
                    rights.append(jnp.concatenate(wanted, axis=1))
                total += jnp.dot(
                    jnp.concatenate(lefts, axis=1),
                    jnp.concatenate(rights, axis=0),
                    preferred_element_type=jnp.float32,
                )
            rounded = total.astype(out.dtype)
            quarters, quarter = out.shape[1], out.shape[4]
            for target in range(slots):
                for q in range(quarters):
                    out[place, q, row, target] = rounded[
                        q * quarter : (q + 1) * quarter, target * tb : (target + 1) * tb
                    ]
        return carry

    lax.fori_loop(0, n_left, one_source, 0)


def on_device(density_tiles, tile_columns):
    rows, groups, slots, tb, _ = density_tiles.shape
    n_x, n_y, n_lo, n_hi = (lax.axis_size(a) for a in ("x", "y", "z_lo", "z_hi"))
    n_z = n_lo * n_hi
    x, y, core = lax.axis_index("x"), lax.axis_index("y"), lax.axis_index("core")
    z = lax.axis_index("z_hi") * n_lo + lax.axis_index("z_lo")
    cores = [(0, 1), (1, 0)]
    exact = tile_columns.astype(jnp.bfloat16)

    def right_payload(group):
        tiles = lax.dynamic_index_in_dim(density_tiles, group, 1, keepdims=False)
        columns = lax.dynamic_index_in_dim(exact, group, 1, keepdims=False)
        return with_tail(tiles, jnp.broadcast_to(columns.reshape(-1, 1), (rows * slots, tb)))

    own = right_payload(2 * x + core)
    other = right_payload(2 * x + 1 - core)
    right = {}
    right[0, 0] = own
    chains = {(0, 1): own, (0, -1): own, (1, 1): other, (1, -1): other}

    def ring(step, keys):
        for flip, way in keys:
            perm = z_steps(way, flip if step == 1 else 0, n_hi, n_lo)
            chains[flip, way] = lax.ppermute(chains[flip, way], ZC, perm)
            right[flip, (-way * step) % n_z] = chains[flip, way]

    half = n_z // 2
    ring(1, [(0, 1), (0, -1), (1, 1), (1, -1)])

    def left_payload(to_y):
        tiles = lax.dynamic_slice_in_dim(density_tiles, 2 * to_y, 2, 1)
        return with_tail(tiles, exact.reshape(rows, groups * slots))

    left = {(0, 0): left_payload(y)}
    for step in range(1, n_y):
        perm = [(s, (s + step) % n_y) for s in range(n_y)]
        left[0, -step % n_y] = lax.ppermute(left_payload((y + step) % n_y), "y", perm)
    right[1, 0] = lax.ppermute(other, "core", cores)
    for step in range(n_y):
        left[1, step] = lax.ppermute(left[0, step], "core", cores)

    for step in range(2, half):
        ring(step, [(0, 1), (0, -1), (1, 1), (1, -1)])
    ring(half, [(0, 1), (1, -1)])

    left_keys = [(flip, step) for flip in range(2) for step in range(n_y)]
    right_keys = [(flip, step) for flip in range(2) for step in range(n_z)]

    columns = jnp.stack(
        [left[k][-TAIL : -TAIL + rows, : groups * slots] for k in left_keys]
    ).astype(jnp.int32)
    columns = columns.reshape(len(left_keys), rows, groups, slots)
    inner = lax.dynamic_slice_in_dim(columns, 2 * y, 2, 2)
    wanted = lax.dynamic_slice_in_dim(columns, 2 * x + core, 1, 2)
    live = inner >= 0
    per_group = rows * n_hi * 2
    local = inner % per_group
    inner_z = (local // (2 * rows)) * n_lo + (inner // per_group) % n_lo
    inner_core = (local // rows) % 2
    source = (inner_core ^ core) * n_z + (inner_z - z) % n_z
    index = jnp.where(live, source * rows + inner % rows, 0)
    left_index = jnp.concatenate([index.reshape(-1), live.astype(jnp.int32).reshape(-1)])
    targets = jnp.where(wanted >= 0, wanted, EMPTY_TARGET).reshape(-1)
    places = jnp.stack([((y + step) % n_y) * 2 + (core ^ flip) for flip, step in left_keys]).astype(jnp.int32)

    n_left, n_right = len(left_keys), len(right_keys)
    left_shape, right_shape = left[0, 0].shape, right[0, 0].shape
    smem = pl.BlockSpec(memory_space=pltpu.SMEM)
    partial = pl.pallas_call(
        functools.partial(products, n_left, n_right, rows, slots),
        out_shape=jax.ShapeDtypeStruct((2 * n_y, n_x, rows, slots, tb // n_x, tb), jnp.bfloat16),
        in_specs=[smem] * 3 + [pl.BlockSpec(memory_space=pl.ANY)] * (n_left + n_right),
        out_specs=pl.BlockSpec(memory_space=pltpu.VMEM),
        scratch_shapes=[
            pltpu.VMEM((n_left, *left_shape), jnp.bfloat16),
            pltpu.VMEM((n_right, *right_shape), jnp.bfloat16),
            pltpu.VMEM((n_right * TAIL, tb), jnp.float32),
            pltpu.SemaphoreType.DMA((n_left,)),
            pltpu.SemaphoreType.DMA((n_right,)),
        ],
    )(left_index, targets, places, *[left[k] for k in left_keys], *[right[k] for k in right_keys])

    arrived = lax.all_to_all(
        partial.reshape(2 * n_y * n_x, rows, slots, tb // n_x, tb),
        ("y", "core", "x"),
        split_axis=0,
        concat_axis=0,
        tiled=True,
    )
    arrived = arrived.reshape(n_y, 2, n_x, rows, slots, tb // n_x, tb)
    total = arrived.astype(jnp.float32).sum(axis=0).astype(jnp.bfloat16)
    return total.transpose(2, 1, 0, 3, 4, 5).reshape(rows, groups, slots, tb // n_x, tb)


def solution(mesh):
    fine = Mesh(mesh.devices.reshape(4, 2, 4, 2, 4), ("y", "z_lo", "z_hi", "core", "x"))
    return jax.shard_map(
        on_device,
        mesh=fine,
        in_specs=(P(ROWS_COLS, None, None, None, None), P(ROWS_COLS, None, None)),
        out_specs=P(ROWS_COLS, None, None, "x", None),
        check_vma=False,
    )
```

```python
import functools

import jax
import jax.numpy as jnp
from jax import lax
from jax.experimental import pallas as pl
from jax.experimental.pallas import tpu as pltpu
from jax.sharding import Mesh
from jax.sharding import PartitionSpec as P


ROWS_COLS = ("y", "z_lo", "z_hi", "core")
ZC = ("z_lo", "z_hi", "core")
TAIL = 16
EMPTY_TARGET = -3


def z_place(z, n_hi, n_lo):
    z = z % (n_hi * n_lo)
    return (z % n_lo) * n_hi + z // n_lo


def z_steps(step, flip, n_hi, n_lo):
    n = n_hi * n_lo
    return [
        (z_place(z, n_hi, n_lo) * 2 + c, z_place(z + step, n_hi, n_lo) * 2 + (c ^ flip))
        for z in range(n)
        for c in range(2)
    ]


def with_tail(tiles, tail_rows):
    tail = jnp.pad(tail_rows, ((0, TAIL - tail_rows.shape[0]), (0, 128 - tail_rows.shape[1])))
    return jnp.concatenate([tiles.reshape(-1, tiles.shape[-1]), tail.astype(tiles.dtype)], axis=0)


def picked(tiles, columns, live, wanted):
    out = []
    for number in wanted:
        total = None
        for tile, column in zip(tiles, columns):
            part = tile * jnp.where(column == number, live, 0.0).astype(tile.dtype)
            total = part if total is None else total + part
        out.append(total)
    return jnp.concatenate(out, axis=1)


def row_product(sizes, left, right, right_columns, index, live, targets, n, row):
    rows, slots, terms, tb = sizes
    i = n * rows + row
    wanted = [targets[i * slots + t].astype(jnp.float32) for t in range(slots)]
    total = None
    for first in range(0, terms, 2):
        lefts, rights = [], []
        for term in (first, first + 1):
            lefts.append(left[n][pl.ds((row * terms + term) * tb, tb), :])
            inner = index[i * terms + term]
            source = inner // rows
            at = (inner - source * rows) * slots
            tiles = [
                right[source, pl.ds(pl.multiple_of((at + slot) * tb, tb), tb), :]
                for slot in range(slots)
            ]
            columns = [right_columns[pl.ds(source * TAIL + at + slot, 1), :] for slot in range(slots)]
            rights.append(picked(tiles, columns, live[i * terms + term].astype(jnp.float32), wanted))
        part = jnp.dot(
            jnp.concatenate(lefts, axis=1),
            jnp.concatenate(rights, axis=0),
            preferred_element_type=jnp.float32,
        )
        total = part if total is None else total + part
    return total


def bring(right_in, right, right_columns, tiles_end):
    for n, ref in enumerate(right_in):
        right[n] = ref[...]
        right_columns[pl.ds(n * TAIL, TAIL), :] = ref[pl.ds(tiles_end, TAIL), :].astype(jnp.float32)


def early_products(n_left, sizes, index, live, targets, *refs):
    rows, slots, _, tb = sizes
    left, right_in = refs[:n_left], refs[n_left:-3]
    out, right, right_columns = refs[-3:]
    bring(right_in, right, right_columns, rows * slots * tb)
    for n in range(n_left):
        for row in range(rows):
            out[n * rows + row] = row_product(
                sizes, left, right, right_columns, index, live, targets, n, row
            )


def late_products(n_left, sizes, index, live, targets, places, early, *refs):
    rows, slots, terms, tb = sizes
    left, right_in = refs[:n_left], refs[n_left:-3]
    out, right, right_columns = refs[-3:]
    bring(right_in, right, right_columns, rows * slots * tb)
    quarters, quarter = out.shape[1], out.shape[4]
    for n in range(n_left):
        place = places[n]

        def write(row, total):
            rounded = total.astype(out.dtype)
            for t in range(slots):
                for q in range(quarters):
                    out[place, q, row, t] = rounded[
                        q * quarter : (q + 1) * quarter, t * tb : (t + 1) * tb
                    ]

        for row in range(rows):
            i = n * rows + row
            hits = sum(live[i * terms + term] for term in range(terms))

            @pl.when(hits > 0)
            def _():
                write(
                    row,
                    early[i]
                    + row_product(sizes, left, right, right_columns, index, live, targets, n, row),
                )

            @pl.when(hits == 0)
            def _():
                write(row, early[i])


def on_device(density_tiles, tile_columns):
    rows, groups, slots, tb, _ = density_tiles.shape
    n_x, n_y, n_lo, n_hi = (lax.axis_size(a) for a in ("x", "y", "z_lo", "z_hi"))
    n_z = n_lo * n_hi
    x, y, core = lax.axis_index("x"), lax.axis_index("y"), lax.axis_index("core")
    z = lax.axis_index("z_hi") * n_lo + lax.axis_index("z_lo")
    cores = [(0, 1), (1, 0)]
    exact = tile_columns.astype(jnp.bfloat16)

    def right_payload(group):
        tiles = lax.dynamic_index_in_dim(density_tiles, group, 1, keepdims=False)
        columns = lax.dynamic_index_in_dim(exact, group, 1, keepdims=False)
        return with_tail(tiles, jnp.broadcast_to(columns.reshape(-1, 1), (rows * slots, tb)))

    own = right_payload(2 * x + core)
    other = right_payload(2 * x + 1 - core)
    right = {}
    right[0, 0] = own
    chains = {(0, 1): own, (0, -1): own, (1, 1): other, (1, -1): other}

    def ring(step, keys):
        for flip, way in keys:
            perm = z_steps(way, flip if step == 1 else 0, n_hi, n_lo)
            chains[flip, way] = lax.ppermute(chains[flip, way], ZC, perm)
            right[flip, (-way * step) % n_z] = chains[flip, way]

    half = n_z // 2
    ring(1, [(0, 1), (0, -1), (1, 1), (1, -1)])

    def left_payload(to_y):
        tiles = lax.dynamic_slice_in_dim(density_tiles, 2 * to_y, 2, 1)
        return with_tail(tiles, exact.reshape(rows, groups * slots))

    left = {(0, 0): left_payload(y)}
    for step in range(1, n_y):
        perm = [(s, (s + step) % n_y) for s in range(n_y)]
        payload = left_payload((y + step) % n_y)
        left[0, -step % n_y] = lax.ppermute(payload, "y", perm)
    right[1, 0] = lax.ppermute(other, "core", cores)
    left[1, 0] = lax.ppermute(left[0, 0], "core", cores)
    for step in range(1, n_y):
        left[1, step] = lax.ppermute(left[0, step], "core", cores)

    for step in range(2, half):
        ring(step, [(0, 1), (0, -1), (1, 1), (1, -1)])
    ring(half, [(0, 1), (1, -1)])

    left_keys = [(flip, step) for flip in range(2) for step in range(n_y)]
    early_keys = [(flip, (half + 1 + n) % n_z) for flip in range(2) for n in range(n_z - 1)]
    late_keys = [(flip, half) for flip in range(2)]

    columns = jnp.stack(
        [left[k][-TAIL : -TAIL + rows, : groups * slots] for k in left_keys]
    ).astype(jnp.int32)
    columns = columns.reshape(len(left_keys), rows, groups, slots)
    inner = lax.dynamic_slice_in_dim(columns, 2 * y, 2, 2)
    wanted = lax.dynamic_slice_in_dim(columns, 2 * x + core, 1, 2)
    listed = inner >= 0
    per_group = rows * n_hi * 2
    local = inner % per_group
    inner_z = (local // (2 * rows)) * n_lo + (inner // per_group) % n_lo
    flip = ((local // rows) % 2) ^ core
    behind = (inner_z - z - half - 1) % n_z
    early = listed & (behind < n_z - 1)
    late = listed & (behind == n_z - 1)
    early_index = jnp.where(early, (flip * (n_z - 1) + behind) * rows + inner % rows, 0).reshape(-1)
    late_index = jnp.where(late, flip * rows + inner % rows, 0).reshape(-1)
    early, late = early.astype(jnp.int32).reshape(-1), late.astype(jnp.int32).reshape(-1)
    targets = jnp.where(wanted >= 0, wanted, EMPTY_TARGET).reshape(-1)
    places = jnp.stack([((y + step) % n_y) * 2 + (core ^ flip) for flip, step in left_keys]).astype(jnp.int32)

    n_left, n_early, n_late = len(left_keys), len(early_keys), len(late_keys)
    sizes = (rows, slots, 2 * slots, tb)
    smem, vmem = pl.BlockSpec(memory_space=pltpu.SMEM), pl.BlockSpec(memory_space=pltpu.VMEM)

    def right_scratch(n):
        return [
            pltpu.VMEM((n, *right[0, 0].shape), jnp.bfloat16),
            pltpu.VMEM((n * TAIL, tb), jnp.float32),
        ]

    lefts = [left[k] for k in left_keys]
    first = pl.pallas_call(
        functools.partial(early_products, n_left, sizes),
        out_shape=jax.ShapeDtypeStruct((n_left * rows, tb, slots * tb), jnp.float32),
        in_specs=[smem] * 3 + [vmem] * (n_left + n_early),
        out_specs=vmem,
        scratch_shapes=right_scratch(n_early),
        cost_estimate=pl.CostEstimate(flops=8 * 10**9, bytes_accessed=9 * 2**20, transcendentals=0),
    )(early_index, early, targets, *lefts, *[right[k] for k in early_keys])
    partial = pl.pallas_call(
        functools.partial(late_products, n_left, sizes),
        out_shape=jax.ShapeDtypeStruct((2 * n_y, n_x, rows, slots, tb // n_x, tb), jnp.bfloat16),
        in_specs=[smem] * 4 + [vmem] * (1 + n_left + n_late),
        out_specs=vmem,
        scratch_shapes=right_scratch(n_late),
    )(late_index, late, targets, places, first, *lefts, *[right[k] for k in late_keys])

    arrived = lax.all_to_all(
        partial.reshape(2 * n_y * n_x, rows, slots, tb // n_x, tb),
        ("y", "core", "x"),
        split_axis=0,
        concat_axis=0,
        tiled=True,
    )
    arrived = arrived.reshape(n_y, 2, n_x, rows, slots, tb // n_x, tb)
    total = arrived.astype(jnp.float32).sum(axis=0).astype(jnp.bfloat16)
    return total.transpose(2, 1, 0, 3, 4, 5).reshape(rows, groups, slots, tb // n_x, tb)


def solution(mesh):
    fine = Mesh(mesh.devices.reshape(4, 2, 4, 2, 4), ("y", "z_lo", "z_hi", "core", "x"))

    return jax.shard_map(
        on_device,
        mesh=fine,
        in_specs=(P(ROWS_COLS, None, None, None, None), P(ROWS_COLS, None, None)),
        out_specs=P(ROWS_COLS, None, None, "x", None),
        check_vma=False,
    )
```

```python
import functools

import jax
import jax.numpy as jnp
from jax import lax
from jax.experimental import pallas as pl
from jax.experimental.pallas import tpu as pltpu
from jax.sharding import Mesh
from jax.sharding import PartitionSpec as P


ROWS_COLS = ("y", "z_lo", "z_hi", "core")
ZC = ("z_lo", "z_hi", "core")
TAIL = 16
VMEM_LIMIT = 16 * 2**20
NO_TARGET = -3


def z_place(z, n_hi, n_lo):
    z = z % (n_hi * n_lo)
    return (z % n_lo) * n_hi + z // n_lo


def z_steps(step, flip, n_hi, n_lo):
    n = n_hi * n_lo
    return [
        (z_place(z, n_hi, n_lo) * 2 + c, z_place(z + step, n_hi, n_lo) * 2 + (c ^ flip))
        for z in range(n)
        for c in range(2)
    ]


def with_tail(tiles, tail_rows):
    tail = jnp.pad(tail_rows, ((0, TAIL - tail_rows.shape[0]), (0, 128 - tail_rows.shape[1])))
    return jnp.concatenate([tiles.reshape(-1, tiles.shape[-1]), tail.astype(tiles.dtype)], axis=0)


def picked(tiles, columns, wanted):
    out = []
    for number in wanted:
        total = None
        for tile, column in zip(tiles, columns):
            part = tile * jnp.where(column == number, 1.0, 0.0).astype(tile.dtype)
            total = part if total is None else total + part
        out.append(total)
    return jnp.concatenate(out, axis=1)


def products(n_left, sizes, columns, own, *refs):
    rows, slots, n_lo, n_hi, tb = sizes
    n_z = n_lo * n_hi
    left, right_in = refs[:n_left], refs[n_left:-4]
    out, right, right_columns, arrived = refs[-4:]
    x, y, z, core = (own[n] for n in range(4))
    quarters, quarter = out.shape[1], out.shape[4]
    copies = [
        pltpu.make_async_copy(ref, right.at[n], arrived.at[n]) for n, ref in enumerate(right_in)
    ]
    for copy in copies:
        copy.start()
    for n, copy in enumerate(copies):
        copy.wait()
        right_columns[pl.ds(n * TAIL, TAIL), :] = right[n, pl.ds(rows * slots * tb, TAIL), :].astype(
            jnp.float32
        )

    def term(n, row, group, slot, wanted):
        i = n * rows + row
        column = columns[i, (n_lo * y + group) * slots + slot]
        live = column >= 0
        local = jnp.where(live, column - (n_lo * y + group) * (rows * 2 * n_hi), 0)
        owner = lax.div(local, rows)
        inner_row = local - owner * rows
        inner_z = lax.div(owner, 2) * n_lo + group
        flip = (owner % 2) ^ core
        source = flip * n_z + lax.rem(inner_z - z + n_z, n_z)
        at = inner_row * slots
        tiles = [
            right[source, pl.ds(pl.multiple_of((at + s) * tb, tb), tb), :] for s in range(slots)
        ]
        listed = [right_columns[pl.ds(source * TAIL + at + s, 1), :] for s in range(slots)]
        numbers = [jnp.where(live & (t >= 0), t, NO_TARGET).astype(jnp.float32) for t in wanted]
        ref_rows = pl.ds((row * n_lo * slots + group * slots + slot) * tb, tb)
        return left[n][ref_rows, :], picked(tiles, listed, numbers)

    for n in range(n_left):
        flip, step = divmod(n, n_left // 2)
        place = lax.rem(y + step, n_left // 2) * 2 + (core ^ flip)
        for row in range(rows):
            wanted = [columns[n * rows + row, (2 * x + core) * slots + t] for t in range(slots)]
            total = None
            for group in range(n_lo):
                pairs = [term(n, row, group, slot, wanted) for slot in range(slots)]
                part = jnp.dot(
                    jnp.concatenate([p[0] for p in pairs], axis=1),
                    jnp.concatenate([p[1] for p in pairs], axis=0),
                    preferred_element_type=jnp.float32,
                )
                total = part if total is None else total + part
            rounded = total.astype(out.dtype)
            for t in range(slots):
                for q in range(quarters):
                    out[place, q, row, t] = rounded[
                        q * quarter : (q + 1) * quarter, t * tb : (t + 1) * tb
                    ]


def on_device(density_tiles, tile_columns):
    rows, groups, slots, tb, _ = density_tiles.shape
    n_x, n_y, n_lo, n_hi = (lax.axis_size(a) for a in ("x", "y", "z_lo", "z_hi"))
    n_z = n_lo * n_hi
    x, y, core = lax.axis_index("x"), lax.axis_index("y"), lax.axis_index("core")
    z = lax.axis_index("z_hi") * n_lo + lax.axis_index("z_lo")
    cores = [(0, 1), (1, 0)]
    exact = tile_columns.astype(jnp.bfloat16)

    def right_payload(group):
        tiles = lax.dynamic_index_in_dim(density_tiles, group, 1, keepdims=False)
        columns = lax.dynamic_index_in_dim(exact, group, 1, keepdims=False)
        return with_tail(tiles, jnp.broadcast_to(columns.reshape(-1, 1), (rows * slots, tb)))

    own = right_payload(2 * x + core)
    other = right_payload(2 * x + 1 - core)
    right = {}
    right[0, 0] = own
    chains = {(0, 1): own, (0, -1): own, (1, 1): other, (1, -1): other}

    def ring(step, keys):
        for flip, way in keys:
            perm = z_steps(way, flip if step == 1 else 0, n_hi, n_lo)
            chains[flip, way] = lax.ppermute(chains[flip, way], ZC, perm)
            right[flip, (-way * step) % n_z] = chains[flip, way]

    half = n_z // 2
    ring(1, [(0, 1), (0, -1), (1, 1), (1, -1)])

    def left_payload(to_y):
        tiles = lax.dynamic_slice_in_dim(density_tiles, 2 * to_y, 2, 1)
        return with_tail(tiles, exact.reshape(rows, groups * slots))

    left = {(0, 0): lax.optimization_barrier(left_payload(y))}
    for step in range(1, n_y):
        perm = [(s, (s + step) % n_y) for s in range(n_y)]
        payload = left_payload((y + step) % n_y)
        left[0, -step % n_y] = lax.ppermute(payload, "y", perm)
    right[1, 0] = lax.ppermute(other, "core", cores)
    left[1, 0] = lax.ppermute(left[0, 0], "core", cores)
    for step in range(1, n_y):
        left[1, step] = lax.ppermute(left[0, step], "core", cores)

    for step in range(2, half):
        ring(step, [(0, 1), (0, -1), (1, 1), (1, -1)])
    ring(half, [(0, 1), (1, -1)])

    left_keys = [(flip, step) for flip in range(2) for step in range(n_y)]
    right_keys = [(flip, step) for flip in range(2) for step in range(n_z)]
    columns = jnp.concatenate(
        [left[k][-TAIL : -TAIL + rows, : groups * slots] for k in left_keys], axis=0
    ).astype(jnp.int32)
    own_place = jnp.stack([x, y, z, core]).astype(jnp.int32)
    smem, vmem = pl.BlockSpec(memory_space=pltpu.SMEM), pl.BlockSpec(memory_space=pltpu.VMEM)
    lefts = [pltpu.with_memory_space_constraint(left[k], pltpu.VMEM) for k in left_keys]
    rights = [pltpu.with_memory_space_constraint(right[k], pltpu.HBM) for k in right_keys]
    partial = pl.pallas_call(
        functools.partial(products, len(left_keys), (rows, slots, n_lo, n_hi, tb)),
        out_shape=pltpu.VMEM((2 * n_y, n_x, rows, slots, tb // n_x, tb), jnp.bfloat16),
        in_specs=[smem] * 2 + [vmem] * len(lefts) + [pl.BlockSpec(memory_space=pltpu.HBM)] * len(rights),
        out_specs=vmem,
        scratch_shapes=[
            pltpu.VMEM((len(right_keys), *right[0, 0].shape), jnp.bfloat16),
            pltpu.VMEM((len(right_keys) * TAIL, tb), jnp.float32),
            pltpu.SemaphoreType.DMA((len(right_keys),)),
        ],
        compiler_params=pltpu.CompilerParams(vmem_limit_bytes=VMEM_LIMIT),
    )(columns, own_place, *lefts, *rights)

    arrived = lax.all_to_all(
        partial.reshape(2 * n_y * n_x, rows, slots, tb // n_x, tb),
        ("y", "core", "x"),
        split_axis=0,
        concat_axis=0,
        tiled=True,
    )
    arrived = arrived.reshape(n_y, 2, n_x, rows, slots, tb // n_x, tb)
    total = arrived.astype(jnp.float32).sum(axis=0).astype(jnp.bfloat16)
    return total.transpose(2, 1, 0, 3, 4, 5).reshape(rows, groups, slots, tb // n_x, tb)


def solution(mesh):
    fine = Mesh(mesh.devices.reshape(4, 2, 4, 2, 4), ("y", "z_lo", "z_hi", "core", "x"))

    return jax.shard_map(
        on_device,
        mesh=fine,
        in_specs=(P(ROWS_COLS, None, None, None, None), P(ROWS_COLS, None, None)),
        out_specs=P(ROWS_COLS, None, None, "x", None),
        check_vma=False,
    )
```

```python
import functools

import jax
import jax.numpy as jnp
from jax import lax
from jax.experimental import pallas as pl
from jax.experimental.pallas import tpu as pltpu
from jax.sharding import Mesh
from jax.sharding import PartitionSpec as P


ROWS_COLS = ("y", "z_lo", "z_hi", "core")
ZC = ("z_lo", "z_hi", "core")
TAIL = 16
NO_TARGET = -3


def z_place(z, n_hi, n_lo):
    z = z % (n_hi * n_lo)
    return (z % n_lo) * n_hi + z // n_lo


def z_steps(step, flip, n_hi, n_lo):
    n = n_hi * n_lo
    return [
        (z_place(z, n_hi, n_lo) * 2 + c, z_place(z + step, n_hi, n_lo) * 2 + (c ^ flip))
        for z in range(n)
        for c in range(2)
    ]


def picked(tiles, columns, wanted):
    out = []
    for number in wanted:
        total = None
        for tile, column in zip(tiles, columns):
            part = tile * jnp.where(column == number, 1.0, 0.0).astype(tile.dtype)
            total = part if total is None else total + part
        out.append(total)
    return jnp.concatenate(out, axis=1)


class Rows:
    def __init__(self, sizes, columns, own):
        self.rows, self.slots, self.n_y, self.n_lo, self.n_hi, self.tb = sizes
        self.columns = columns
        self.x, self.y, self.z, self.core = (own[n] for n in range(4))

    def all(self):
        return [(n, row) for n in range(2 * self.n_y) for row in range(self.rows)]

    def place(self, n):
        flip, step = divmod(n, self.n_y)
        return lax.rem(self.y + step, self.n_y) * 2 + (self.core ^ flip)

    def wanted(self, n, row):
        at = (2 * self.x + self.core) * self.slots
        return [self.columns[n * self.rows + row, at + t] for t in range(self.slots)]

    def inner(self, n, row, group, slot):
        n_z = self.n_lo * self.n_hi
        first = self.n_lo * self.y + group
        column = self.columns[n * self.rows + row, first * self.slots + slot]
        listed = column >= 0
        local = jnp.where(listed, column - first * (self.rows * 2 * self.n_hi), 0)
        owner = lax.div(local, self.rows)
        inner_z = lax.div(owner, 2) * self.n_lo + group
        behind = lax.rem(inner_z - self.z - n_z // 2 - 1 + 2 * n_z, n_z)
        source = (lax.rem(owner, 2) ^ self.core) * n_z + behind
        return listed, source, (local - owner * self.rows) * self.slots

    def product(self, left, right, right_columns, n, row):
        tb, slots = self.tb, self.slots
        wanted = self.wanted(n, row)
        total = None
        for group in range(self.n_lo):
            lefts, rights = [], []
            for slot in range(slots):
                here, source, at = self.inner(n, row, group, slot)
                tiles = [
                    right[source, pl.ds(pl.multiple_of((at + s) * tb, tb), tb), :]
                    for s in range(slots)
                ]
                listed = [right_columns[pl.ds(source * TAIL + at + s, 1), :] for s in range(slots)]
                numbers = [
                    jnp.where(here & (wanted[t] >= 0), wanted[t], NO_TARGET).astype(jnp.float32)
                    for t in range(slots)
                ]
                rows = pl.ds(((row * self.n_lo + group) * slots + slot) * tb, tb)
                lefts.append(left[n][rows, :])
                rights.append(picked(tiles, listed, numbers))
            part = jnp.dot(
                jnp.concatenate(lefts, axis=1),
                jnp.concatenate(rights, axis=0),
                preferred_element_type=jnp.float32,
            )
            total = part if total is None else total + part
        return total


def first_payloads(places, columns, tiles, own, other, left_tail, held, arrived, listed):
    rows, groups, slots, tb, _ = tiles.shape
    copies = [
        pltpu.make_async_copy(tiles.at[row, places[g], slot], out.at[pl.ds((row * slots + slot) * tb, tb)], arrived)
        for g, out in enumerate((own, other))
        for row in range(rows)
        for slot in range(slots)
    ]
    fetch = pltpu.make_async_copy(columns, held, listed)
    fetch.start()
    for copy in copies:
        copy.start()
    fetch.wait()
    line = lax.broadcasted_iota(jnp.int32, (TAIL, tb), 0)
    lane = lax.broadcasted_iota(jnp.int32, (TAIL, tb), 1)
    numbers = [held[row].astype(jnp.float32) for row in range(rows)]
    for g, out in enumerate((own, other)):
        tail = jnp.zeros((TAIL, tb), jnp.float32)
        chosen = lax.broadcasted_iota(jnp.int32, (slots, groups), 1) == places[g]
        for row in range(rows):
            of_group = jnp.sum(jnp.where(chosen, numbers[row], 0.0), axis=1, keepdims=True)
            for slot in range(slots):
                number = jnp.broadcast_to(of_group[slot : slot + 1], (TAIL, tb))
                tail = jnp.where(line == row * slots + slot, number, tail)
        out[pl.ds(rows * slots * tb, TAIL), :] = tail.astype(out.dtype)
    tail = jnp.zeros((TAIL, tb), jnp.float32)
    for row in range(rows):
        for g in range(groups):
            for slot in range(slots):
                number = jnp.broadcast_to(numbers[row][slot : slot + 1, g : g + 1], (TAIL, tb))
                tail = jnp.where((line == row) & (lane == g * slots + slot), number, tail)
    left_tail[...] = tail.astype(left_tail.dtype)
    for copy in copies:
        copy.wait()


def listed_columns(rows, *refs):
    left, out = refs[:-1], refs[-1]
    for n, ref in enumerate(left):
        tail = ref[pl.ds(ref.shape[0] - TAIL, TAIL), :].astype(jnp.float32).astype(jnp.int32)
        out[pl.ds(n * rows, rows), :] = tail[:rows]


def products(sizes, columns, own, *refs):
    work = Rows(sizes, columns, own)
    n_left, tb = 2 * work.n_y, work.tb
    left, right_in = refs[:n_left], refs[n_left:-4]
    out, right, right_columns, arrived = refs[-4:]
    copies = [
        pltpu.make_async_copy(ref, right.at[n], arrived.at[n]) for n, ref in enumerate(right_in)
    ]
    for copy in copies:
        copy.start()
    for n, copy in enumerate(copies):
        copy.wait()
        tail = right[n, pl.ds(work.rows * work.slots * tb, TAIL), :]
        right_columns[pl.ds(n * TAIL, TAIL), :] = tail.astype(jnp.float32)
    quarters, quarter = out.shape[1], out.shape[4]
    for n, row in work.all():
        rounded = work.product(left, right, right_columns, n, row).astype(out.dtype)
        for t in range(work.slots):
            for q in range(quarters):
                out[work.place(n), q, row, t] = rounded[
                    q * quarter : (q + 1) * quarter, t * tb : (t + 1) * tb
                ]


def final_sum(n_y, arrived, out):
    rows, groups, slots = out.shape[:3]
    for g in range(groups):
        x, core = divmod(g, 2)
        for row in range(rows):
            for t in range(slots):
                total = arrived[0, core, x, row, t].astype(jnp.float32)
                for y in range(1, n_y):
                    total += arrived[y, core, x, row, t].astype(jnp.float32)
                out[row, g, t] = total.astype(out.dtype)


def on_device(density_tiles, tile_columns):
    rows, groups, slots, tb, _ = density_tiles.shape
    n_x, n_y, n_lo, n_hi = (lax.axis_size(a) for a in ("x", "y", "z_lo", "z_hi"))
    n_z = n_lo * n_hi
    x, y, core = lax.axis_index("x"), lax.axis_index("y"), lax.axis_index("core")
    z = lax.axis_index("z_hi") * n_lo + lax.axis_index("z_lo")
    cores = [(0, 1), (1, 0)]

    smem, vmem = pl.BlockSpec(memory_space=pltpu.SMEM), pl.BlockSpec(memory_space=pltpu.VMEM)
    hbm = pl.BlockSpec(memory_space=pltpu.HBM)
    limit = pltpu.CompilerParams(vmem_limit_bytes=4 * 2**20)
    payload = (rows * slots * tb + TAIL, tb)
    own, other, left_tail = pl.pallas_call(
        first_payloads,
        out_shape=[pltpu.VMEM(shape, jnp.bfloat16) for shape in (payload, payload, (TAIL, tb))],
        in_specs=[smem, hbm, hbm],
        out_specs=[vmem] * 3,
        scratch_shapes=[
            pltpu.VMEM((rows, slots, groups), jnp.int32),
            pltpu.SemaphoreType.DMA,
            pltpu.SemaphoreType.DMA,
        ],
        compiler_params=limit,
    )(
        jnp.stack([2 * x + core, 2 * x + 1 - core]).astype(jnp.int32),
        pltpu.with_memory_space_constraint(tile_columns.transpose(0, 2, 1), pltpu.HBM),
        pltpu.with_memory_space_constraint(density_tiles, pltpu.HBM),
    )
    right = {}
    right[0, 0] = own
    chains = {(0, 1): own, (0, -1): own, (1, 1): other, (1, -1): other}

    def ring(step, keys):
        for flip, way in keys:
            perm = z_steps(way, flip if step == 1 else 0, n_hi, n_lo)
            chains[flip, way] = lax.ppermute(chains[flip, way], ZC, perm)
            right[flip, (-way * step) % n_z] = chains[flip, way]

    half = n_z // 2
    ring(1, [(0, 1), (0, -1), (1, 1), (1, -1)])

    def left_payload(to_y):
        tiles = lax.dynamic_slice_in_dim(density_tiles, 2 * to_y, 2, 1)
        return jnp.concatenate([tiles.reshape(-1, tb), left_tail], axis=0)

    left = {(0, 0): lax.optimization_barrier(left_payload(y))}
    for step in (2, 1, 3):
        perm = [(s, (s + step) % n_y) for s in range(n_y)]
        sent = left_payload((y + step) % n_y)
        left[0, -step % n_y] = lax.ppermute(sent, "y", perm)
    right[1, 0] = lax.ppermute(other, "core", cores)
    left[1, 0] = lax.ppermute(left[0, 0], "core", cores)
    for step in range(1, n_y):
        left[1, step] = lax.ppermute(left[0, step], "core", cores)

    for step in range(2, half):
        ring(step, [(0, 1), (0, -1), (1, 1), (1, -1)])
    ring(half, [(0, 1), (1, -1)])

    left_keys = [(flip, step) for flip in range(2) for step in range(n_y)]
    sizes = (rows, slots, n_y, n_lo, n_hi, tb)
    quarter = tb // n_x

    rights = [right[flip, (n + half + 1) % n_z] for flip in range(2) for n in range(n_z)]
    lefts = [pltpu.with_memory_space_constraint(left[k], pltpu.VMEM) for k in left_keys]
    rights = [pltpu.with_memory_space_constraint(r, pltpu.HBM) for r in rights]
    columns = pl.pallas_call(
        functools.partial(listed_columns, rows),
        out_shape=jax.ShapeDtypeStruct((len(lefts) * rows, tb), jnp.int32),
        in_specs=[vmem] * len(lefts),
        out_specs=vmem,
        compiler_params=limit,
    )(*lefts)
    partial = pl.pallas_call(
        functools.partial(products, sizes),
        out_shape=pltpu.VMEM((2 * n_y, n_x, rows, slots, quarter, tb), jnp.bfloat16),
        in_specs=[smem] * 2 + [vmem] * len(lefts) + [hbm] * len(rights),
        out_specs=vmem,
        scratch_shapes=[
            pltpu.VMEM((len(rights), *payload), jnp.bfloat16),
            pltpu.VMEM((len(rights) * TAIL, tb), jnp.float32),
            pltpu.SemaphoreType.DMA((len(rights),)),
        ],
        compiler_params=pltpu.CompilerParams(vmem_limit_bytes=12 * 2**20),
    )(columns, jnp.stack([x, y, z, core]).astype(jnp.int32), *lefts, *rights)

    arrived = lax.all_to_all(
        partial.reshape(2 * n_y * n_x, rows, slots, quarter, tb),
        ("y", "core", "x"),
        split_axis=0,
        concat_axis=0,
        tiled=True,
    )
    arrived = arrived.reshape(n_y, 2, n_x, rows, slots, quarter, tb)
    return pl.pallas_call(
        functools.partial(final_sum, n_y),
        out_shape=jax.ShapeDtypeStruct((rows, groups, slots, quarter, tb), jnp.bfloat16),
        in_specs=[vmem],
        out_specs=vmem,
        compiler_params=limit,
    )(pltpu.with_memory_space_constraint(arrived, pltpu.VMEM))


def solution(mesh):
    fine = Mesh(mesh.devices.reshape(4, 2, 4, 2, 4), ("y", "z_lo", "z_hi", "core", "x"))

    return jax.shard_map(
        on_device,
        mesh=fine,
        in_specs=(P(ROWS_COLS, None, None, None, None), P(ROWS_COLS, None, None)),
        out_specs=P(ROWS_COLS, None, None, "x", None),
        check_vma=False,
    )
```

```python
import functools

import jax
import jax.numpy as jnp
from jax import lax
from jax.experimental import pallas as pl
from jax.experimental.pallas import tpu as pltpu
from jax.sharding import Mesh
from jax.sharding import PartitionSpec as P


ROWS_COLS = ("y", "z_lo", "z_hi", "core")
ZC = ("z_lo", "z_hi", "core")
TAIL = 16
NO_TARGET = -3


def z_place(z, n_hi, n_lo):
    z = z % (n_hi * n_lo)
    return (z % n_lo) * n_hi + z // n_lo


def z_steps(step, flip, n_hi, n_lo):
    n = n_hi * n_lo
    return [
        (z_place(z, n_hi, n_lo) * 2 + c, z_place(z + step, n_hi, n_lo) * 2 + (c ^ flip))
        for z in range(n)
        for c in range(2)
    ]


def picked(tiles, columns, wanted):
    out = []
    for number in wanted:
        total = None
        for tile, column in zip(tiles, columns):
            part = tile * jnp.where(column == number, 1.0, 0.0).astype(tile.dtype)
            total = part if total is None else total + part
        out.append(total)
    return jnp.concatenate(out, axis=1)


class Rows:
    def __init__(self, sizes, columns, own):
        self.rows, self.slots, self.n_y, self.n_lo, self.n_hi, self.tb = sizes
        self.columns = columns
        self.x, self.y, self.z, self.core = (own[n] for n in range(4))

    def all(self):
        return [(n, row) for n in range(2 * self.n_y) for row in range(self.rows)]

    def place(self, n):
        flip, y = divmod(n, self.n_y)
        return y * 2 + (self.core ^ flip)

    def wanted(self, n, row):
        at = (2 * self.x + self.core) * self.slots
        return [self.columns[n * self.rows + row, at + t] for t in range(self.slots)]

    def inner(self, n, row, group, slot):
        n_z = self.n_lo * self.n_hi
        first = self.n_lo * self.y + group
        column = self.columns[n * self.rows + row, first * self.slots + slot]
        listed = column >= 0
        local = jnp.where(listed, column - first * (self.rows * 2 * self.n_hi), 0)
        owner = lax.div(local, self.rows)
        inner_z = lax.div(owner, 2) * self.n_lo + group
        behind = lax.rem(inner_z - self.z - n_z // 2 - 1 + 2 * n_z, n_z)
        source = (lax.rem(owner, 2) ^ self.core) * n_z + behind
        return listed, source, (local - owner * self.rows) * self.slots

    def product(self, left, right, right_columns, n, row):
        tb, slots = self.tb, self.slots
        wanted = self.wanted(n, row)
        total = None
        for group in range(self.n_lo):
            lefts, rights = [], []
            for slot in range(slots):
                here, source, at = self.inner(n, row, group, slot)
                tiles = [
                    right[source, pl.ds(pl.multiple_of((at + s) * tb, tb), tb), :]
                    for s in range(slots)
                ]
                listed = [right_columns[pl.ds(source * TAIL + at + s, 1), :] for s in range(slots)]
                numbers = [
                    jnp.where(here & (wanted[t] >= 0), wanted[t], NO_TARGET).astype(jnp.float32)
                    for t in range(slots)
                ]
                rows = pl.ds(((row * self.n_lo + group) * slots + slot) * tb, tb)
                flip, y = divmod(n, self.n_y)
                lefts.append(left[flip][y, rows, :])
                rights.append(picked(tiles, listed, numbers))
            part = jnp.dot(
                jnp.concatenate(lefts, axis=1),
                jnp.concatenate(rights, axis=0),
                preferred_element_type=jnp.float32,
            )
            total = part if total is None else total + part
        return total


def first_payloads(places, columns, tiles, own, other, left_tail, held, arrived, listed):
    rows, groups, slots, tb, _ = tiles.shape
    copies = [
        pltpu.make_async_copy(tiles.at[row, places[g], slot], out.at[pl.ds((row * slots + slot) * tb, tb)], arrived)
        for g, out in enumerate((own, other))
        for row in range(rows)
        for slot in range(slots)
    ]
    fetch = pltpu.make_async_copy(columns, held, listed)
    fetch.start()
    for copy in copies:
        copy.start()
    fetch.wait()
    line = lax.broadcasted_iota(jnp.int32, (TAIL, tb), 0)
    lane = lax.broadcasted_iota(jnp.int32, (TAIL, tb), 1)
    numbers = [held[row].astype(jnp.float32) for row in range(rows)]
    for g, out in enumerate((own, other)):
        tail = jnp.zeros((TAIL, tb), jnp.float32)
        chosen = lax.broadcasted_iota(jnp.int32, (slots, groups), 1) == places[g]
        for row in range(rows):
            of_group = jnp.sum(jnp.where(chosen, numbers[row], 0.0), axis=1, keepdims=True)
            for slot in range(slots):
                number = jnp.broadcast_to(of_group[slot : slot + 1], (TAIL, tb))
                tail = jnp.where(line == row * slots + slot, number, tail)
        out[pl.ds(rows * slots * tb, TAIL), :] = tail.astype(out.dtype)
    tail = jnp.zeros((TAIL, tb), jnp.float32)
    for row in range(rows):
        for g in range(groups):
            for slot in range(slots):
                number = jnp.broadcast_to(numbers[row][slot : slot + 1, g : g + 1], (TAIL, tb))
                tail = jnp.where((line == row) & (lane == g * slots + slot), number, tail)
    left_tail[...] = tail.astype(left_tail.dtype)
    for copy in copies:
        copy.wait()


def listed_columns(rows, *refs):
    left, out = refs[:-1], refs[-1]
    n_y, lines = left[0].shape[:2]
    for flip, ref in enumerate(left):
        for y in range(n_y):
            tail = ref[y, pl.ds(lines - TAIL, TAIL), :].astype(jnp.float32).astype(jnp.int32)
            out[pl.ds((flip * n_y + y) * rows, rows), :] = tail[:rows]


def products(sizes, columns, own, *refs):
    work = Rows(sizes, columns, own)
    tb = work.tb
    left, right_in = refs[:2], refs[2:-4]
    out, right, right_columns, arrived = refs[-4:]
    copies = [
        pltpu.make_async_copy(ref, right.at[n], arrived.at[n]) for n, ref in enumerate(right_in)
    ]
    for copy in copies:
        copy.start()
    for n, copy in enumerate(copies):
        copy.wait()
        tail = right[n, pl.ds(work.rows * work.slots * tb, TAIL), :]
        right_columns[pl.ds(n * TAIL, TAIL), :] = tail.astype(jnp.float32)
    quarters, quarter = out.shape[1], out.shape[4]
    for n, row in work.all():
        rounded = work.product(left, right, right_columns, n, row).astype(out.dtype)
        for t in range(work.slots):
            for q in range(quarters):
                out[work.place(n), q, row, t] = rounded[
                    q * quarter : (q + 1) * quarter, t * tb : (t + 1) * tb
                ]


def final_sum(n_y, arrived, out):
    rows, groups, slots = out.shape[:3]
    for g in range(groups):
        x, core = divmod(g, 2)
        for row in range(rows):
            for t in range(slots):
                total = arrived[0, core, x, row, t].astype(jnp.float32)
                for y in range(1, n_y):
                    total += arrived[y, core, x, row, t].astype(jnp.float32)
                out[row, g, t] = total.astype(out.dtype)


def on_device(density_tiles, tile_columns):
    rows, groups, slots, tb, _ = density_tiles.shape
    n_x, n_y, n_lo, n_hi = (lax.axis_size(a) for a in ("x", "y", "z_lo", "z_hi"))
    n_z = n_lo * n_hi
    x, y, core = lax.axis_index("x"), lax.axis_index("y"), lax.axis_index("core")
    z = lax.axis_index("z_hi") * n_lo + lax.axis_index("z_lo")
    cores = [(0, 1), (1, 0)]

    smem, vmem = pl.BlockSpec(memory_space=pltpu.SMEM), pl.BlockSpec(memory_space=pltpu.VMEM)
    hbm = pl.BlockSpec(memory_space=pltpu.HBM)
    limit = pltpu.CompilerParams(vmem_limit_bytes=4 * 2**20)
    payload = (rows * slots * tb + TAIL, tb)
    own, other, left_tail = pl.pallas_call(
        first_payloads,
        out_shape=[pltpu.VMEM(shape, jnp.bfloat16) for shape in (payload, payload, (TAIL, tb))],
        in_specs=[smem, hbm, hbm],
        out_specs=[vmem] * 3,
        scratch_shapes=[
            pltpu.VMEM((rows, slots, groups), jnp.int32),
            pltpu.SemaphoreType.DMA,
            pltpu.SemaphoreType.DMA,
        ],
        compiler_params=limit,
    )(
        jnp.stack([2 * x + core, 2 * x + 1 - core]).astype(jnp.int32),
        pltpu.with_memory_space_constraint(tile_columns.transpose(0, 2, 1), pltpu.HBM),
        pltpu.with_memory_space_constraint(density_tiles, pltpu.HBM),
    )
    right = {}
    right[0, 0] = own
    chains = {(0, 1): own, (0, -1): own, (1, 1): other, (1, -1): other}

    def ring(step, keys):
        for flip, way in keys:
            perm = z_steps(way, flip if step == 1 else 0, n_hi, n_lo)
            chains[flip, way] = lax.ppermute(chains[flip, way], ZC, perm)
            right[flip, (-way * step) % n_z] = chains[flip, way]

    half = n_z // 2
    ring(1, [(0, 1), (0, -1), (1, 1), (1, -1)])

    by_y = density_tiles.reshape(rows, n_y, -1, tb).transpose(1, 0, 2, 3).reshape(n_y, -1, tb)
    tails = jnp.broadcast_to(left_tail, (n_y, TAIL, tb))
    packed = jnp.concatenate([by_y, tails], axis=1)
    left = [lax.all_to_all(packed, "y", split_axis=0, concat_axis=0, tiled=True)]
    right[1, 0] = lax.ppermute(other, "core", cores)
    left.append(lax.ppermute(left[0], "core", cores))

    for step in range(2, half):
        ring(step, [(0, 1), (0, -1), (1, 1), (1, -1)])
    ring(half, [(0, 1), (1, -1)])

    sizes = (rows, slots, n_y, n_lo, n_hi, tb)
    quarter = tb // n_x

    rights = [right[flip, (n + half + 1) % n_z] for flip in range(2) for n in range(n_z)]
    lefts = [pltpu.with_memory_space_constraint(a, pltpu.VMEM) for a in left]
    rights = [pltpu.with_memory_space_constraint(r, pltpu.HBM) for r in rights]
    columns = pl.pallas_call(
        functools.partial(listed_columns, rows),
        out_shape=jax.ShapeDtypeStruct((2 * n_y * rows, tb), jnp.int32),
        in_specs=[vmem] * len(lefts),
        out_specs=vmem,
        compiler_params=limit,
    )(*lefts)
    partial = pl.pallas_call(
        functools.partial(products, sizes),
        out_shape=pltpu.VMEM((2 * n_y, n_x, rows, slots, quarter, tb), jnp.bfloat16),
        in_specs=[smem] * 2 + [vmem] * len(lefts) + [hbm] * len(rights),
        out_specs=vmem,
        scratch_shapes=[
            pltpu.VMEM((len(rights), *payload), jnp.bfloat16),
            pltpu.VMEM((len(rights) * TAIL, tb), jnp.float32),
            pltpu.SemaphoreType.DMA((len(rights),)),
        ],
        compiler_params=pltpu.CompilerParams(vmem_limit_bytes=12 * 2**20),
    )(columns, jnp.stack([x, y, z, core]).astype(jnp.int32), *lefts, *rights)

    arrived = lax.all_to_all(
        partial.reshape(2 * n_y * n_x, rows, slots, quarter, tb),
        ("y", "core", "x"),
        split_axis=0,
        concat_axis=0,
        tiled=True,
    )
    arrived = arrived.reshape(n_y, 2, n_x, rows, slots, quarter, tb)
    return pl.pallas_call(
        functools.partial(final_sum, n_y),
        out_shape=jax.ShapeDtypeStruct((rows, groups, slots, quarter, tb), jnp.bfloat16),
        in_specs=[vmem],
        out_specs=vmem,
        compiler_params=limit,
    )(pltpu.with_memory_space_constraint(arrived, pltpu.VMEM))


def solution(mesh):
    fine = Mesh(mesh.devices.reshape(4, 2, 4, 2, 4), ("y", "z_lo", "z_hi", "core", "x"))

    return jax.shard_map(
        on_device,
        mesh=fine,
        in_specs=(P(ROWS_COLS, None, None, None, None), P(ROWS_COLS, None, None)),
        out_specs=P(ROWS_COLS, None, None, "x", None),
        check_vma=False,
    )
```

```python
import functools

import jax
import jax.numpy as jnp
from jax import lax
from jax.experimental import pallas as pl
from jax.experimental.pallas import tpu as pltpu
from jax.sharding import Mesh
from jax.sharding import PartitionSpec as P


ROWS_COLS = ("y", "z_lo", "z_hi", "core")
ZC = ("z_lo", "z_hi", "core")
TAIL = 16
NO_TARGET = -3


def z_place(z, n_hi, n_lo):
    z = z % (n_hi * n_lo)
    return (z % n_lo) * n_hi + z // n_lo


def z_steps(step, flip, n_hi, n_lo):
    n = n_hi * n_lo
    return [
        (z_place(z, n_hi, n_lo) * 2 + c, z_place(z + step, n_hi, n_lo) * 2 + (c ^ flip))
        for z in range(n)
        for c in range(2)
    ]


def picked(tiles, columns, wanted):
    out = []
    for number in wanted:
        total = None
        for tile, column in zip(tiles, columns):
            part = tile * jnp.where(column == number, 1.0, 0.0).astype(tile.dtype)
            total = part if total is None else total + part
        out.append(total)
    return jnp.concatenate(out, axis=1)


class Rows:
    def __init__(self, sizes, columns):
        self.rows, self.slots, self.n_y, self.n_lo, self.n_hi, self.tb = sizes
        self.columns = columns
        place = 2 * self.n_y * self.rows
        self.x, self.y, self.z, self.core = (columns[place + n, 0] for n in range(4))

    def all(self):
        return [(n, row) for n in range(2 * self.n_y) for row in range(self.rows)]

    def place(self, n):
        flip, y = divmod(n, self.n_y)
        return y * 2 + (self.core ^ flip)

    def wanted(self, n, row):
        at = (2 * self.x + self.core) * self.slots
        return [self.columns[n * self.rows + row, at + t] for t in range(self.slots)]

    def inner(self, n, row, group, slot):
        n_z = self.n_lo * self.n_hi
        first = self.n_lo * self.y + group
        column = self.columns[n * self.rows + row, first * self.slots + slot]
        listed = column >= 0
        local = jnp.where(listed, column - first * (self.rows * 2 * self.n_hi), 0)
        owner = lax.div(local, self.rows)
        inner_z = lax.div(owner, 2) * self.n_lo + group
        behind = lax.rem(inner_z - self.z - n_z // 2 - 1 + 2 * n_z, n_z)
        source = (lax.rem(owner, 2) ^ self.core) * n_z + behind
        return listed, source, (local - owner * self.rows) * self.slots

    def product(self, left, right, right_columns, n, row):
        tb, slots = self.tb, self.slots
        wanted = self.wanted(n, row)
        total = None
        for group in range(self.n_lo):
            lefts, rights = [], []
            for slot in range(slots):
                here, source, at = self.inner(n, row, group, slot)
                tiles = [
                    right[source, pl.ds(pl.multiple_of((at + s) * tb, tb), tb), :]
                    for s in range(slots)
                ]
                listed = [right_columns[pl.ds(source * TAIL + at + s, 1), :] for s in range(slots)]
                numbers = [
                    jnp.where(here & (wanted[t] >= 0), wanted[t], NO_TARGET).astype(jnp.float32)
                    for t in range(slots)
                ]
                rows = pl.ds(((row * self.n_lo + group) * slots + slot) * tb, tb)
                flip, y = divmod(n, self.n_y)
                lefts.append(left[flip][y, rows, :])
                rights.append(picked(tiles, listed, numbers))
            part = jnp.dot(
                jnp.concatenate(lefts, axis=1),
                jnp.concatenate(rights, axis=0),
                preferred_element_type=jnp.float32,
            )
            total = part if total is None else total + part
        return total


def first_payloads(places, columns, tiles, own, other, left_tail, held, arrived, listed):
    rows, groups, slots, tb, _ = tiles.shape
    copies = [
        pltpu.make_async_copy(tiles.at[row, places[g], slot], out.at[pl.ds((row * slots + slot) * tb, tb)], arrived)
        for g, out in enumerate((own, other))
        for row in range(rows)
        for slot in range(slots)
    ]
    fetch = pltpu.make_async_copy(columns, held, listed)
    fetch.start()
    for copy in copies:
        copy.start()
    fetch.wait()
    line = lax.broadcasted_iota(jnp.int32, (TAIL, tb), 0)
    lane = lax.broadcasted_iota(jnp.int32, (TAIL, tb), 1)
    numbers = [held[row].astype(jnp.float32) for row in range(rows)]
    for g, out in enumerate((own, other)):
        tail = jnp.zeros((TAIL, tb), jnp.float32)
        chosen = lax.broadcasted_iota(jnp.int32, (slots, groups), 1) == places[g]
        for row in range(rows):
            of_group = jnp.sum(jnp.where(chosen, numbers[row], 0.0), axis=1, keepdims=True)
            for slot in range(slots):
                number = jnp.broadcast_to(of_group[slot : slot + 1], (TAIL, tb))
                tail = jnp.where(line == row * slots + slot, number, tail)
        out[pl.ds(rows * slots * tb, TAIL), :] = tail.astype(out.dtype)
    tail = jnp.zeros((TAIL, tb), jnp.float32)
    for row in range(rows):
        for g in range(groups):
            for slot in range(slots):
                number = jnp.broadcast_to(numbers[row][slot : slot + 1, g : g + 1], (TAIL, tb))
                tail = jnp.where((line == row) & (lane == g * slots + slot), number, tail)
    left_tail[...] = tail.astype(left_tail.dtype)
    for copy in copies:
        copy.wait()


def listed_columns(rows, place, *refs):
    left, out = refs[:-1], refs[-1]
    for n in range(4):
        out[pl.ds(2 * left[0].shape[0] * rows + n, 1), :] = jnp.full((1, out.shape[1]), place[n], jnp.int32)
    n_y, lines = left[0].shape[:2]
    for flip, ref in enumerate(left):
        for y in range(n_y):
            tail = ref[y, pl.ds(lines - TAIL, TAIL), :].astype(jnp.float32).astype(jnp.int32)
            out[pl.ds((flip * n_y + y) * rows, rows), :] = tail[:rows]


def products(sizes, columns_in, *refs):
    left, right_in = refs[:2], refs[2:-6]
    out, right, right_columns, arrived, columns, listed = refs[-6:]
    fetch = pltpu.make_async_copy(columns_in, columns, listed)
    fetch.start()
    copies = [
        pltpu.make_async_copy(ref, right.at[n], arrived.at[n]) for n, ref in enumerate(right_in)
    ]
    for copy in copies:
        copy.start()
    fetch.wait()
    work = Rows(sizes, columns)
    tb = work.tb
    for n, copy in enumerate(copies):
        copy.wait()
        tail = right[n, pl.ds(work.rows * work.slots * tb, TAIL), :]
        right_columns[pl.ds(n * TAIL, TAIL), :] = tail.astype(jnp.float32)
    quarters, quarter = out.shape[1], out.shape[4]
    for n, row in work.all():
        rounded = work.product(left, right, right_columns, n, row).astype(out.dtype)
        for t in range(work.slots):
            for q in range(quarters):
                out[work.place(n), q, row, t] = rounded[
                    q * quarter : (q + 1) * quarter, t * tb : (t + 1) * tb
                ]


def final_sum(n_y, arrived, out):
    rows, groups, slots = out.shape[:3]
    for g in range(groups):
        x, core = divmod(g, 2)
        for row in range(rows):
            for t in range(slots):
                total = arrived[0, core, x, row, t].astype(jnp.float32)
                for y in range(1, n_y):
                    total += arrived[y, core, x, row, t].astype(jnp.float32)
                out[row, g, t] = total.astype(out.dtype)


def on_device(density_tiles, tile_columns):
    rows, groups, slots, tb, _ = density_tiles.shape
    n_x, n_y, n_lo, n_hi = (lax.axis_size(a) for a in ("x", "y", "z_lo", "z_hi"))
    n_z = n_lo * n_hi
    x, y, core = lax.axis_index("x"), lax.axis_index("y"), lax.axis_index("core")
    z = lax.axis_index("z_hi") * n_lo + lax.axis_index("z_lo")
    cores = [(0, 1), (1, 0)]

    smem, vmem = pl.BlockSpec(memory_space=pltpu.SMEM), pl.BlockSpec(memory_space=pltpu.VMEM)
    hbm = pl.BlockSpec(memory_space=pltpu.HBM)
    limit = pltpu.CompilerParams(vmem_limit_bytes=4 * 2**20)
    payload = (rows * slots * tb + TAIL, tb)
    own, other, left_tail = pl.pallas_call(
        first_payloads,
        out_shape=[pltpu.VMEM(shape, jnp.bfloat16) for shape in (payload, payload, (TAIL, tb))],
        in_specs=[smem, hbm, hbm],
        out_specs=[vmem] * 3,
        scratch_shapes=[
            pltpu.VMEM((rows, slots, groups), jnp.int32),
            pltpu.SemaphoreType.DMA,
            pltpu.SemaphoreType.DMA,
        ],
        compiler_params=limit,
    )(
        jnp.stack([2 * x + core, 2 * x + 1 - core]).astype(jnp.int32),
        pltpu.with_memory_space_constraint(tile_columns.transpose(0, 2, 1), pltpu.HBM),
        pltpu.with_memory_space_constraint(density_tiles, pltpu.HBM),
    )
    right = {}
    right[0, 0] = own
    chains = {(0, 1): own, (0, -1): own, (1, 1): other, (1, -1): other}

    def ring(step, keys):
        for flip, way in keys:
            perm = z_steps(way, flip if step == 1 else 0, n_hi, n_lo)
            chains[flip, way] = lax.ppermute(chains[flip, way], ZC, perm)
            right[flip, (-way * step) % n_z] = chains[flip, way]

    half = n_z // 2
    ring(1, [(0, 1), (0, -1), (1, 1), (1, -1)])

    by_y = density_tiles.reshape(rows, n_y, -1, tb).transpose(1, 0, 2, 3).reshape(n_y, -1, tb)
    tails = jnp.broadcast_to(left_tail, (n_y, TAIL, tb))
    packed = jnp.concatenate([by_y, tails], axis=1)
    left = [lax.all_to_all(packed, "y", split_axis=0, concat_axis=0, tiled=True)]
    right[1, 0] = lax.ppermute(other, "core", cores)
    left.append(lax.ppermute(left[0], "core", cores))

    for step in range(2, half):
        ring(step, [(0, 1), (0, -1), (1, 1), (1, -1)])
    ring(half, [(0, 1), (1, -1)])

    sizes = (rows, slots, n_y, n_lo, n_hi, tb)
    quarter = tb // n_x

    rights = [right[flip, (n + half + 1) % n_z] for flip in range(2) for n in range(n_z)]
    lefts = [pltpu.with_memory_space_constraint(a, pltpu.VMEM) for a in left]
    rights = [pltpu.with_memory_space_constraint(r, pltpu.HBM) for r in rights]
    columns = pl.pallas_call(
        functools.partial(listed_columns, rows),
        out_shape=pltpu.VMEM((2 * n_y * rows + 8, tb), jnp.int32),
        in_specs=[smem] + [vmem] * len(lefts),
        out_specs=vmem,
        compiler_params=limit,
    )(jnp.stack([x, y, z, core]).astype(jnp.int32), *lefts)
    partial = pl.pallas_call(
        functools.partial(products, sizes),
        out_shape=pltpu.VMEM((2 * n_y, n_x, rows, slots, quarter, tb), jnp.bfloat16),
        in_specs=[vmem] * (1 + len(lefts)) + [hbm] * len(rights),
        out_specs=vmem,
        scratch_shapes=[
            pltpu.VMEM((len(rights), *payload), jnp.bfloat16),
            pltpu.VMEM((len(rights) * TAIL, tb), jnp.float32),
            pltpu.SemaphoreType.DMA((len(rights),)),
            pltpu.SMEM((2 * n_y * rows + 8, tb), jnp.int32),
            pltpu.SemaphoreType.DMA,
        ],
        compiler_params=pltpu.CompilerParams(vmem_limit_bytes=12 * 2**20),
    )(pltpu.with_memory_space_constraint(columns, pltpu.VMEM), *lefts, *rights)

    arrived = lax.all_to_all(
        partial.reshape(2 * n_y * n_x, rows, slots, quarter, tb),
        ("y", "core", "x"),
        split_axis=0,
        concat_axis=0,
        tiled=True,
    )
    arrived = arrived.reshape(n_y, 2, n_x, rows, slots, quarter, tb)
    return pl.pallas_call(
        functools.partial(final_sum, n_y),
        out_shape=jax.ShapeDtypeStruct((rows, groups, slots, quarter, tb), jnp.bfloat16),
        in_specs=[vmem],
        out_specs=vmem,
        compiler_params=limit,
    )(pltpu.with_memory_space_constraint(arrived, pltpu.VMEM))


def solution(mesh):
    fine = Mesh(mesh.devices.reshape(4, 2, 4, 2, 4), ("y", "z_lo", "z_hi", "core", "x"))

    return jax.shard_map(
        on_device,
        mesh=fine,
        in_specs=(P(ROWS_COLS, None, None, None, None), P(ROWS_COLS, None, None)),
        out_specs=P(ROWS_COLS, None, None, "x", None),
        check_vma=False,
    )
```

```python
import functools

import jax
import jax.numpy as jnp
from jax import lax
from jax.experimental import pallas as pl
from jax.experimental.pallas import tpu as pltpu
from jax.sharding import Mesh
from jax.sharding import PartitionSpec as P


ROWS_COLS = ("y", "z_lo", "z_hi", "core")
ZC = ("z_lo", "z_hi", "core")
TAIL = 16
NO_TARGET = -3


def z_place(z, n_hi, n_lo):
    z = z % (n_hi * n_lo)
    return (z % n_lo) * n_hi + z // n_lo


def z_pairs(odd, flip, n_hi, n_lo):
    n = n_hi * n_lo
    pairs = []
    for z in range(n):
        to = z + 1 if (z + odd) % 2 == 0 else z - 1
        pairs += [
            (z_place(z, n_hi, n_lo) * 2 + c, z_place(to, n_hi, n_lo) * 2 + (c ^ flip)) for c in range(2)
        ]
    return pairs


def picked(tiles, columns, wanted):
    out = []
    for number in wanted:
        total = None
        for tile, column in zip(tiles, columns):
            part = tile * jnp.where(column == number, 1.0, 0.0).astype(tile.dtype)
            total = part if total is None else total + part
        out.append(total)
    return jnp.concatenate(out, axis=1)


class Rows:
    def __init__(self, sizes, columns):
        self.rows, self.slots, self.n_y, self.n_lo, self.n_hi, self.tb = sizes
        self.columns = columns
        place = 2 * self.n_y * self.rows
        self.x, self.y, self.z, self.core = (columns[place + n, 0] for n in range(4))

    def all(self):
        return [(n, row) for n in range(2 * self.n_y) for row in range(self.rows)]

    def place(self, n):
        flip, step = divmod(n, self.n_y)
        return lax.rem(self.y + step, self.n_y) * 2 + (self.core ^ flip)

    def wanted(self, n, row):
        at = (2 * self.x + self.core) * self.slots
        return [self.columns[n * self.rows + row, at + t] for t in range(self.slots)]

    def inner(self, n, row, group, slot):
        n_z = self.n_lo * self.n_hi
        first = self.n_lo * self.y + group
        column = self.columns[n * self.rows + row, first * self.slots + slot]
        listed = column >= 0
        local = jnp.where(listed, column - first * (self.rows * 2 * self.n_hi), 0)
        owner = lax.div(local, self.rows)
        inner_z = lax.div(owner, 2) * self.n_lo + group
        ahead = lax.rem(inner_z - self.z + n_z, n_z)
        steps = jnp.minimum(ahead, n_z - ahead)
        chain = lax.rem(self.z + steps + jnp.where(ahead < n_z // 2, 1, 0), 2)
        at = jnp.where(ahead == 0, 0, jnp.where(ahead == n_z // 2, n_z - 1, 2 * steps - 1 + chain))
        source = (lax.rem(owner, 2) ^ self.core) * n_z + at
        return listed, source, (local - owner * self.rows) * self.slots

    def product(self, left, right, right_columns, n, row):
        tb, slots = self.tb, self.slots
        wanted = self.wanted(n, row)
        total = None
        for group in range(self.n_lo):
            lefts, rights = [], []
            for slot in range(slots):
                here, source, at = self.inner(n, row, group, slot)
                tiles = [
                    right[source, pl.ds(pl.multiple_of((at + s) * tb, tb), tb), :]
                    for s in range(slots)
                ]
                listed = [right_columns[pl.ds(source * TAIL + at + s, 1), :] for s in range(slots)]
                numbers = [
                    jnp.where(here & (wanted[t] >= 0), wanted[t], NO_TARGET).astype(jnp.float32)
                    for t in range(slots)
                ]
                rows = pl.ds(((row * self.n_lo + group) * slots + slot) * tb, tb)
                lefts.append(left[n][rows, :])
                rights.append(picked(tiles, listed, numbers))
            part = jnp.dot(
                jnp.concatenate(lefts, axis=1),
                jnp.concatenate(rights, axis=0),
                preferred_element_type=jnp.float32,
            )
            total = part if total is None else total + part
        return total


def first_payloads(places, columns, tiles, own, other, left_tail, held, arrived, listed):
    rows, groups, slots, tb, _ = tiles.shape
    copies = [
        pltpu.make_async_copy(tiles.at[row, places[g], slot], out.at[pl.ds((row * slots + slot) * tb, tb)], arrived)
        for g, out in enumerate((own, other))
        for row in range(rows)
        for slot in range(slots)
    ]
    fetch = pltpu.make_async_copy(columns, held, listed)
    fetch.start()
    for copy in copies:
        copy.start()
    fetch.wait()
    line = lax.broadcasted_iota(jnp.int32, (TAIL, tb), 0)
    lane = lax.broadcasted_iota(jnp.int32, (TAIL, tb), 1)
    numbers = [held[row].astype(jnp.float32) for row in range(rows)]
    for g, out in enumerate((own, other)):
        tail = jnp.zeros((TAIL, tb), jnp.float32)
        chosen = lax.broadcasted_iota(jnp.int32, (slots, groups), 1) == places[g]
        for row in range(rows):
            of_group = jnp.sum(jnp.where(chosen, numbers[row], 0.0), axis=1, keepdims=True)
            for slot in range(slots):
                number = jnp.broadcast_to(of_group[slot : slot + 1], (TAIL, tb))
                tail = jnp.where(line == row * slots + slot, number, tail)
        out[pl.ds(rows * slots * tb, TAIL), :] = tail.astype(out.dtype)
    tail = jnp.zeros((TAIL, tb), jnp.float32)
    for row in range(rows):
        for g in range(groups):
            for slot in range(slots):
                number = jnp.broadcast_to(numbers[row][slot : slot + 1, g : g + 1], (TAIL, tb))
                tail = jnp.where((line == row) & (lane == g * slots + slot), number, tail)
    left_tail[...] = tail.astype(left_tail.dtype)
    for copy in copies:
        copy.wait()


def listed_columns(rows, place, *refs):
    left, out = refs[:-1], refs[-1]
    for n in range(4):
        out[pl.ds(len(left) * rows + n, 1), :] = jnp.full((1, out.shape[1]), place[n], jnp.int32)
    for n, ref in enumerate(left):
        tail = ref[pl.ds(ref.shape[0] - TAIL, TAIL), :].astype(jnp.float32).astype(jnp.int32)
        out[pl.ds(n * rows, rows), :] = tail[:rows]


def products(n_left, sizes, columns_in, *refs):
    left, right_in = refs[:n_left], refs[n_left:-6]
    out, right, right_columns, arrived, columns, listed = refs[-6:]
    fetch = pltpu.make_async_copy(columns_in, columns, listed)
    fetch.start()
    copies = [
        pltpu.make_async_copy(ref, right.at[n], arrived.at[n]) for n, ref in enumerate(right_in)
    ]
    for copy in copies:
        copy.start()
    fetch.wait()
    work = Rows(sizes, columns)
    tb = work.tb
    for n, copy in enumerate(copies):
        copy.wait()
        tail = right[n, pl.ds(work.rows * work.slots * tb, TAIL), :]
        right_columns[pl.ds(n * TAIL, TAIL), :] = tail.astype(jnp.float32)
    quarters, quarter = out.shape[1], out.shape[4]
    for n, row in work.all():
        rounded = work.product(left, right, right_columns, n, row).astype(out.dtype)
        for t in range(work.slots):
            for q in range(quarters):
                out[work.place(n), q, row, t] = rounded[
                    q * quarter : (q + 1) * quarter, t * tb : (t + 1) * tb
                ]


def final_sum(n_y, arrived, out):
    rows, groups, slots = out.shape[:3]
    for g in range(groups):
        x, core = divmod(g, 2)
        for row in range(rows):
            for t in range(slots):
                total = arrived[0, core, x, row, t].astype(jnp.float32)
                for y in range(1, n_y):
                    total += arrived[y, core, x, row, t].astype(jnp.float32)
                out[row, g, t] = total.astype(out.dtype)


def on_device(density_tiles, tile_columns):
    rows, groups, slots, tb, _ = density_tiles.shape
    n_x, n_y, n_lo, n_hi = (lax.axis_size(a) for a in ("x", "y", "z_lo", "z_hi"))
    n_z = n_lo * n_hi
    x, y, core = lax.axis_index("x"), lax.axis_index("y"), lax.axis_index("core")
    z = lax.axis_index("z_hi") * n_lo + lax.axis_index("z_lo")
    cores = [(0, 1), (1, 0)]

    smem, vmem = pl.BlockSpec(memory_space=pltpu.SMEM), pl.BlockSpec(memory_space=pltpu.VMEM)
    hbm = pl.BlockSpec(memory_space=pltpu.HBM)
    limit = pltpu.CompilerParams(vmem_limit_bytes=4 * 2**20)
    payload = (rows * slots * tb + TAIL, tb)
    own, other, left_tail = pl.pallas_call(
        first_payloads,
        out_shape=[pltpu.VMEM(shape, jnp.bfloat16) for shape in (payload, payload, (TAIL, tb))],
        in_specs=[smem, hbm, hbm],
        out_specs=[vmem] * 3,
        scratch_shapes=[
            pltpu.VMEM((rows, slots, groups), jnp.int32),
            pltpu.SemaphoreType.DMA,
            pltpu.SemaphoreType.DMA,
        ],
        compiler_params=limit,
    )(
        jnp.stack([2 * x + core, 2 * x + 1 - core]).astype(jnp.int32),
        pltpu.with_memory_space_constraint(tile_columns.transpose(0, 2, 1), pltpu.HBM),
        pltpu.with_memory_space_constraint(density_tiles, pltpu.HBM),
    )
    right = {(0, 0, 0): own}
    held = {(flip, chain): (own, other)[flip] for flip in range(2) for chain in range(2)}

    def ring(step, keys):
        for flip, chain in keys:
            perm = z_pairs((chain + step - 1) % 2, flip if step == 1 else 0, n_hi, n_lo)
            held[flip, chain] = lax.ppermute(held[flip, chain], ZC, perm)
            right[flip, step, chain] = held[flip, chain]

    half = n_z // 2
    every = [(flip, chain) for flip in range(2) for chain in range(2)]
    ring(1, every)

    def left_payload(to_y):
        tiles = lax.dynamic_slice_in_dim(density_tiles, 2 * to_y, 2, 1)
        return jnp.concatenate([tiles.reshape(-1, tb), left_tail], axis=0)

    left = {(0, 0): lax.optimization_barrier(left_payload(y))}
    for step in (2, 1, 3):
        perm = [(s, (s + step) % n_y) for s in range(n_y)]
        sent = left_payload((y + step) % n_y)
        left[0, -step % n_y] = lax.ppermute(sent, "y", perm)
    right[1, 0, 0] = lax.ppermute(other, "core", cores)
    left[1, 0] = lax.ppermute(left[0, 0], "core", cores)
    for step in range(1, n_y):
        left[1, step] = lax.ppermute(left[0, step], "core", cores)

    for step in range(2, half):
        ring(step, every)
    ring(half, [(0, 0), (1, 1)])

    left_keys = [(flip, step) for flip in range(2) for step in range(n_y)]
    sizes = (rows, slots, n_y, n_lo, n_hi, tb)
    quarter = tb // n_x

    rights = [
        right[key]
        for flip in range(2)
        for key in [(flip, 0, 0)]
        + [(flip, step, chain) for step in range(1, half) for chain in range(2)]
        + [(flip, half, flip)]
    ]
    lefts = [pltpu.with_memory_space_constraint(left[k], pltpu.VMEM) for k in left_keys]
    rights = [pltpu.with_memory_space_constraint(r, pltpu.HBM) for r in rights]
    columns = pl.pallas_call(
        functools.partial(listed_columns, rows),
        out_shape=pltpu.VMEM((2 * n_y * rows + 8, tb), jnp.int32),
        in_specs=[smem] + [vmem] * len(lefts),
        out_specs=vmem,
        compiler_params=limit,
    )(jnp.stack([x, y, z, core]).astype(jnp.int32), *lefts)
    partial = pl.pallas_call(
        functools.partial(products, len(lefts), sizes),
        out_shape=pltpu.VMEM((2 * n_y, n_x, rows, slots, quarter, tb), jnp.bfloat16),
        in_specs=[vmem] * (1 + len(lefts)) + [hbm] * len(rights),
        out_specs=vmem,
        scratch_shapes=[
            pltpu.VMEM((len(rights), *payload), jnp.bfloat16),
            pltpu.VMEM((len(rights) * TAIL, tb), jnp.float32),
            pltpu.SemaphoreType.DMA((len(rights),)),
            pltpu.SMEM((2 * n_y * rows + 8, tb), jnp.int32),
            pltpu.SemaphoreType.DMA,
        ],
        compiler_params=pltpu.CompilerParams(vmem_limit_bytes=12 * 2**20),
    )(pltpu.with_memory_space_constraint(columns, pltpu.VMEM), *lefts, *rights)

    arrived = lax.all_to_all(
        partial.reshape(2 * n_y * n_x, rows, slots, quarter, tb),
        ("y", "core", "x"),
        split_axis=0,
        concat_axis=0,
        tiled=True,
    )
    arrived = arrived.reshape(n_y, 2, n_x, rows, slots, quarter, tb)
    return pl.pallas_call(
        functools.partial(final_sum, n_y),
        out_shape=jax.ShapeDtypeStruct((rows, groups, slots, quarter, tb), jnp.bfloat16),
        in_specs=[vmem],
        out_specs=vmem,
        compiler_params=limit,
    )(pltpu.with_memory_space_constraint(arrived, pltpu.VMEM))


def solution(mesh):
    fine = Mesh(mesh.devices.reshape(4, 2, 4, 2, 4), ("y", "z_lo", "z_hi", "core", "x"))

    return jax.shard_map(
        on_device,
        mesh=fine,
        in_specs=(P(ROWS_COLS, None, None, None, None), P(ROWS_COLS, None, None)),
        out_specs=P(ROWS_COLS, None, None, "x", None),
        check_vma=False,
    )
```

```python
import functools

import jax
import jax.numpy as jnp
from jax import lax
from jax.experimental import pallas as pl
from jax.experimental.pallas import tpu as pltpu
from jax.sharding import Mesh
from jax.sharding import PartitionSpec as P


ROWS_COLS = ("y", "z_lo", "z_hi", "core")
ZC = ("z_lo", "z_hi", "core")
TAIL = 16
NO_TARGET = -3


def z_place(z, n_hi, n_lo):
    z = z % (n_hi * n_lo)
    return (z % n_lo) * n_hi + z // n_lo


def z_pairs(odd, flip, n_hi, n_lo):
    n = n_hi * n_lo
    pairs = []
    for z in range(n):
        to = z + 1 if (z + odd) % 2 == 0 else z - 1
        pairs += [
            (z_place(z, n_hi, n_lo) * 2 + c, z_place(to, n_hi, n_lo) * 2 + (c ^ flip)) for c in range(2)
        ]
    return pairs


def picked(tiles, columns, wanted):
    out = []
    for number in wanted:
        total = None
        for tile, column in zip(tiles, columns):
            part = tile * jnp.where(column == number, 1.0, 0.0).astype(tile.dtype)
            total = part if total is None else total + part
        out.append(total)
    return jnp.concatenate(out, axis=1)


class Rows:
    def __init__(self, sizes, columns):
        self.rows, self.slots, self.n_y, self.n_lo, self.n_hi, self.tb = sizes
        self.columns = columns
        place = 2 * self.n_y * self.rows
        self.x, self.y, self.z, self.core = (columns[place + n, 0] for n in range(4))

    def all(self):
        return [(n, row) for n in range(2 * self.n_y) for row in range(self.rows)]

    def place(self, n):
        flip, step = divmod(n, self.n_y)
        return lax.rem(self.y + step, self.n_y) * 2 + (self.core ^ flip)

    def wanted(self, n, row):
        at = (2 * self.x + self.core) * self.slots
        return [self.columns[n * self.rows + row, at + t] for t in range(self.slots)]

    def inner(self, n, row, group, slot):
        n_z = self.n_lo * self.n_hi
        first = self.n_lo * self.y + group
        column = self.columns[n * self.rows + row, first * self.slots + slot]
        listed = column >= 0
        local = jnp.where(listed, column - first * (self.rows * 2 * self.n_hi), 0)
        owner = lax.div(local, self.rows)
        inner_z = lax.div(owner, 2) * self.n_lo + group
        ahead = lax.rem(inner_z - self.z + n_z, n_z)
        steps = jnp.minimum(ahead, n_z - ahead)
        chain = lax.rem(self.z + steps + jnp.where(ahead < n_z // 2, 1, 0), 2)
        at = jnp.where(ahead == 0, 0, jnp.where(ahead == n_z // 2, n_z - 1, 2 * steps - 1 + chain))
        source = (lax.rem(owner, 2) ^ self.core) * n_z + at
        return listed, source, (local - owner * self.rows) * self.slots

    def product(self, left, right, right_columns, n, row):
        tb, slots = self.tb, self.slots
        wanted = self.wanted(n, row)
        total = None
        for group in range(self.n_lo):
            lefts, rights = [], []
            for slot in range(slots):
                here, source, at = self.inner(n, row, group, slot)
                tiles = [
                    right[source, pl.ds(pl.multiple_of((at + s) * tb, tb), tb), :]
                    for s in range(slots)
                ]
                listed = [right_columns[pl.ds(source * TAIL + at + s, 1), :] for s in range(slots)]
                numbers = [
                    jnp.where(here & (wanted[t] >= 0), wanted[t], NO_TARGET).astype(jnp.float32)
                    for t in range(slots)
                ]
                rows = pl.ds(((row * self.n_lo + group) * slots + slot) * tb, tb)
                lefts.append(left[n][rows, :])
                rights.append(picked(tiles, listed, numbers))
            part = jnp.dot(
                jnp.concatenate(lefts, axis=1),
                jnp.concatenate(rights, axis=0),
                preferred_element_type=jnp.float32,
            )
            total = part if total is None else total + part
        return total


def first_payloads(place, columns, tiles, own, other, left_tail, held, arrived, listed):
    rows, groups, slots, tb, _ = tiles.shape
    copies = [
        pltpu.make_async_copy(tiles.at[row, place[4 + g], slot], out.at[pl.ds((row * slots + slot) * tb, tb)], arrived)
        for g, out in enumerate((own, other))
        for row in range(rows)
        for slot in range(slots)
    ]
    fetch = pltpu.make_async_copy(columns, held, listed)
    fetch.start()
    for copy in copies:
        copy.start()
    fetch.wait()
    line = lax.broadcasted_iota(jnp.int32, (TAIL, tb), 0)
    lane = lax.broadcasted_iota(jnp.int32, (TAIL, tb), 1)
    numbers = [held[row].astype(jnp.float32) for row in range(rows)]
    for g, out in enumerate((own, other)):
        tail = jnp.zeros((TAIL, tb), jnp.float32)
        chosen = lax.broadcasted_iota(jnp.int32, (slots, groups), 1) == place[4 + g]
        for row in range(rows):
            of_group = jnp.sum(jnp.where(chosen, numbers[row], 0.0), axis=1, keepdims=True)
            for slot in range(slots):
                number = jnp.broadcast_to(of_group[slot : slot + 1], (TAIL, tb))
                tail = jnp.where(line == row * slots + slot, number, tail)
        out[pl.ds(rows * slots * tb, TAIL), :] = tail.astype(out.dtype)
    tail = jnp.zeros((TAIL, tb), jnp.float32)
    for row in range(rows):
        for g in range(groups):
            for slot in range(slots):
                number = jnp.broadcast_to(numbers[row][slot : slot + 1, g : g + 1], (TAIL, tb))
                tail = jnp.where((line == row) & (lane == g * slots + slot), number, tail)
    left_tail[...] = tail.astype(left_tail.dtype)
    for copy in copies:
        copy.wait()


def left_payloads(n_y, place, tiles, left_tail, *outs):
    rows, groups, slots, tb, _ = tiles.shape
    per_y = groups // n_y
    for step, out in enumerate(outs):
        to_y = lax.rem(place[1] + step, n_y)
        for row in range(rows):
            for g in range(per_y):
                for slot in range(slots):
                    at = ((row * per_y + g) * slots + slot) * tb
                    out[pl.ds(at, tb), :] = tiles[row, to_y * per_y + g, slot]
        out[pl.ds(rows * per_y * slots * tb, TAIL), :] = left_tail[...]


def listed_columns(rows, place, *refs):
    left, out = refs[:-1], refs[-1]
    for n in range(4):
        out[pl.ds(len(left) * rows + n, 1), :] = jnp.full((1, out.shape[1]), place[n], jnp.int32)
    for n, ref in enumerate(left):
        tail = ref[pl.ds(ref.shape[0] - TAIL, TAIL), :].astype(jnp.float32).astype(jnp.int32)
        out[pl.ds(n * rows, rows), :] = tail[:rows]


def products(n_left, sizes, columns_in, *refs):
    left, right_in = refs[:n_left], refs[n_left:-5]
    out, right, right_columns, columns, listed = refs[-5:]
    fetch = pltpu.make_async_copy(columns_in, columns, listed)
    fetch.start()
    tiles_end = right.shape[1]
    for n, ref in enumerate(right_in):
        right[n] = ref[pl.ds(0, tiles_end), :]
        right_columns[pl.ds(n * TAIL, TAIL), :] = ref[pl.ds(tiles_end, TAIL), :].astype(jnp.float32)
    fetch.wait()
    work = Rows(sizes, columns)
    tb = work.tb
    quarters, quarter = out.shape[1], out.shape[4]
    for n, row in work.all():
        rounded = work.product(left, right, right_columns, n, row).astype(out.dtype)
        for t in range(work.slots):
            for q in range(quarters):
                out[work.place(n), q, row, t] = rounded[
                    q * quarter : (q + 1) * quarter, t * tb : (t + 1) * tb
                ]


def final_sum(n_y, arrived, out):
    rows, groups, slots = out.shape[:3]
    for g in range(groups):
        x, core = divmod(g, 2)
        for row in range(rows):
            for t in range(slots):
                total = arrived[0, core, x, row, t].astype(jnp.float32)
                for y in range(1, n_y):
                    total += arrived[y, core, x, row, t].astype(jnp.float32)
                out[row, g, t] = total.astype(out.dtype)


def on_device(density_tiles, tile_columns):
    rows, groups, slots, tb, _ = density_tiles.shape
    n_x, n_y, n_lo, n_hi = (lax.axis_size(a) for a in ("x", "y", "z_lo", "z_hi"))
    n_z = n_lo * n_hi
    x, y, core = lax.axis_index("x"), lax.axis_index("y"), lax.axis_index("core")
    z = lax.axis_index("z_hi") * n_lo + lax.axis_index("z_lo")
    cores = [(0, 1), (1, 0)]

    smem, vmem = pl.BlockSpec(memory_space=pltpu.SMEM), pl.BlockSpec(memory_space=pltpu.VMEM)
    hbm = pl.BlockSpec(memory_space=pltpu.HBM)
    limit = pltpu.CompilerParams(vmem_limit_bytes=4 * 2**20)
    payload = (rows * slots * tb + TAIL, tb)
    place = jnp.zeros((6,), jnp.int32)
    for n, number in enumerate((x, y, z, core, 2 * x + core, 2 * x + 1 - core)):
        place = jnp.where(lax.iota(jnp.int32, 6) == n, number, place)
    own, other, left_tail = pl.pallas_call(
        first_payloads,
        out_shape=[pltpu.VMEM(shape, jnp.bfloat16) for shape in (payload, payload, (TAIL, tb))],
        in_specs=[smem, hbm, hbm],
        out_specs=[vmem] * 3,
        scratch_shapes=[pltpu.VMEM((rows, slots, groups), jnp.int32), pltpu.SemaphoreType.DMA, pltpu.SemaphoreType.DMA],
        compiler_params=limit,
    )(
        place,
        pltpu.with_memory_space_constraint(tile_columns.transpose(0, 2, 1), pltpu.HBM),
        pltpu.with_memory_space_constraint(density_tiles, pltpu.HBM),
    )
    right = {(0, 0, 0): own}
    held = {(flip, chain): (own, other)[flip] for flip in range(2) for chain in range(2)}

    def ring(step, keys):
        for flip, chain in keys:
            perm = z_pairs((chain + step - 1) % 2, flip if step == 1 else 0, n_hi, n_lo)
            held[flip, chain] = lax.ppermute(held[flip, chain], ZC, perm)
            right[flip, step, chain] = held[flip, chain]

    half = n_z // 2
    every = [(flip, chain) for flip in range(2) for chain in range(2)]
    ring(1, every)

    left_payload = (rows * groups // n_y * slots * tb + TAIL, tb)
    sent = pl.pallas_call(
        functools.partial(left_payloads, n_y),
        out_shape=[pltpu.VMEM(left_payload, jnp.bfloat16)] * n_y,
        in_specs=[smem, vmem, vmem],
        out_specs=[vmem] * n_y,
        compiler_params=limit,
    )(place, *[pltpu.with_memory_space_constraint(a, pltpu.VMEM) for a in (density_tiles, left_tail)])
    left = {(0, 0): sent[0]}
    for step in (2, 1, 3):
        perm = [(s, (s + step) % n_y) for s in range(n_y)]
        left[0, -step % n_y] = lax.ppermute(sent[step], "y", perm)
    right[1, 0, 0] = lax.ppermute(other, "core", cores)
    left[1, 0] = lax.ppermute(left[0, 0], "core", cores)
    for step in range(1, n_y):
        left[1, step] = lax.ppermute(left[0, step], "core", cores)

    for step in range(2, half):
        ring(step, every)
    ring(half, [(0, 0), (1, 1)])

    left_keys = [(flip, step) for flip in range(2) for step in range(n_y)]
    sizes = (rows, slots, n_y, n_lo, n_hi, tb)
    quarter = tb // n_x

    rights = [
        right[key]
        for flip in range(2)
        for key in [(flip, 0, 0)]
        + [(flip, step, chain) for step in range(1, half) for chain in range(2)]
        + [(flip, half, flip)]
    ]
    lefts = [pltpu.with_memory_space_constraint(left[k], pltpu.VMEM) for k in left_keys]
    rights = [pltpu.with_memory_space_constraint(r, pltpu.VMEM) for r in rights]
    columns = pl.pallas_call(
        functools.partial(listed_columns, rows),
        out_shape=pltpu.VMEM((2 * n_y * rows + 8, tb), jnp.int32),
        in_specs=[smem] + [vmem] * len(lefts),
        out_specs=vmem,
        compiler_params=limit,
    )(place, *lefts)
    partial = pl.pallas_call(
        functools.partial(products, len(lefts), sizes),
        out_shape=pltpu.VMEM((2 * n_y, n_x, rows, slots, quarter, tb), jnp.bfloat16),
        in_specs=[vmem] * (1 + len(lefts) + len(rights)),
        out_specs=vmem,
        scratch_shapes=[
            pltpu.VMEM((len(rights), payload[0] - TAIL, tb), jnp.bfloat16),
            pltpu.VMEM((len(rights) * TAIL, tb), jnp.float32),
            pltpu.SMEM((2 * n_y * rows + 8, tb), jnp.int32),
            pltpu.SemaphoreType.DMA,
        ],
        compiler_params=pltpu.CompilerParams(vmem_limit_bytes=12 * 2**20),
    )(pltpu.with_memory_space_constraint(columns, pltpu.VMEM), *lefts, *rights)

    arrived = lax.all_to_all(
        partial.reshape(2 * n_y * n_x, rows, slots, quarter, tb),
        ("y", "core", "x"),
        split_axis=0,
        concat_axis=0,
        tiled=True,
    )
    arrived = arrived.reshape(n_y, 2, n_x, rows, slots, quarter, tb)
    return pl.pallas_call(
        functools.partial(final_sum, n_y),
        out_shape=jax.ShapeDtypeStruct((rows, groups, slots, quarter, tb), jnp.bfloat16),
        in_specs=[vmem],
        out_specs=vmem,
        compiler_params=limit,
    )(pltpu.with_memory_space_constraint(arrived, pltpu.VMEM))


def solution(mesh):
    fine = Mesh(mesh.devices.reshape(4, 2, 4, 2, 4), ("y", "z_lo", "z_hi", "core", "x"))

    return jax.shard_map(
        on_device,
        mesh=fine,
        in_specs=(P(ROWS_COLS, None, None, None, None), P(ROWS_COLS, None, None)),
        out_specs=P(ROWS_COLS, None, None, "x", None),
        check_vma=False,
    )
```

```python
import functools

import jax
import jax.numpy as jnp
from jax import lax
from jax.experimental import pallas as pl
from jax.experimental.pallas import tpu as pltpu
from jax.sharding import Mesh
from jax.sharding import PartitionSpec as P


ROWS_COLS = ("y", "z_lo", "z_hi", "core")
ZC = ("z_lo", "z_hi", "core")
TAIL = 8
NO_TARGET = -3


def z_place(z, n_hi, n_lo):
    z = z % (n_hi * n_lo)
    return (z % n_lo) * n_hi + z // n_lo


def z_pairs(odd, flip, n_hi, n_lo):
    n = n_hi * n_lo
    pairs = []
    for z in range(n):
        to = z + 1 if (z + odd) % 2 == 0 else z - 1
        pairs += [
            (z_place(z, n_hi, n_lo) * 2 + c, z_place(to, n_hi, n_lo) * 2 + (c ^ flip)) for c in range(2)
        ]
    return pairs


def picked(tiles, columns, wanted):
    out = []
    for number in wanted:
        total = None
        for tile, column in zip(tiles, columns):
            part = tile * jnp.where(column == number, 1.0, 0.0).astype(tile.dtype)
            total = part if total is None else total + part
        out.append(total)
    return jnp.concatenate(out, axis=1)


class Rows:
    def __init__(self, sizes, columns):
        self.rows, self.slots, self.n_y, self.n_lo, self.n_hi, self.tb = sizes
        self.columns = columns
        place = 2 * self.n_y * self.rows
        self.x, self.y, self.z, self.core = (columns[place + n, 0] for n in range(4))

    def all(self):
        return [(n, row) for n in range(2 * self.n_y) for row in range(self.rows)]

    def place(self, n):
        flip, step = divmod(n, self.n_y)
        return lax.rem(self.y + step, self.n_y) * 2 + (self.core ^ flip)

    def wanted(self, n, row):
        at = (2 * self.x + self.core) * self.slots
        return [self.columns[n * self.rows + row, at + t] for t in range(self.slots)]

    def inner(self, n, row, group, slot):
        n_z = self.n_lo * self.n_hi
        first = self.n_lo * self.y + group
        column = self.columns[n * self.rows + row, first * self.slots + slot]
        listed = column >= 0
        local = jnp.where(listed, column - first * (self.rows * 2 * self.n_hi), 0)
        owner = lax.div(local, self.rows)
        inner_z = lax.div(owner, 2) * self.n_lo + group
        ahead = lax.rem(inner_z - self.z + n_z, n_z)
        steps = jnp.minimum(ahead, n_z - ahead)
        chain = lax.rem(self.z + steps + jnp.where(ahead < n_z // 2, 1, 0), 2)
        at = jnp.where(ahead == 0, 0, jnp.where(ahead == n_z // 2, n_z - 1, 2 * steps - 1 + chain))
        source = (lax.rem(owner, 2) ^ self.core) * n_z + at
        return listed, source, (local - owner * self.rows) * self.slots

    def product(self, left, right, right_columns, n, row):
        tb, slots = self.tb, self.slots
        wanted = self.wanted(n, row)
        total = None
        for group in range(self.n_lo):
            lefts, rights = [], []
            for slot in range(slots):
                here, source, at = self.inner(n, row, group, slot)
                tiles = [
                    right[source, pl.ds(pl.multiple_of((at + s) * tb, tb), tb), :]
                    for s in range(slots)
                ]
                listed = [right_columns[pl.ds(source * TAIL + at + s, 1), :] for s in range(slots)]
                numbers = [
                    jnp.where(here & (wanted[t] >= 0), wanted[t], NO_TARGET).astype(jnp.float32)
                    for t in range(slots)
                ]
                rows = pl.ds(((row * self.n_lo + group) * slots + slot) * tb, tb)
                lefts.append(left[n][rows, :])
                rights.append(picked(tiles, listed, numbers))
            part = jnp.dot(
                jnp.concatenate(lefts, axis=1),
                jnp.concatenate(rights, axis=0),
                preferred_element_type=jnp.float32,
            )
            total = part if total is None else total + part
        return total


def first_payloads(place, columns, tiles, own, other, left_tail, held, arrived, listed):
    rows, groups, slots, tb, _ = tiles.shape
    copies = [
        pltpu.make_async_copy(tiles.at[row, place[4 + g], slot], out.at[pl.ds((row * slots + slot) * tb, tb)], arrived)
        for g, out in enumerate((own, other))
        for row in range(rows)
        for slot in range(slots)
    ]
    fetch = pltpu.make_async_copy(columns, held, listed)
    fetch.start()
    for copy in copies:
        copy.start()
    fetch.wait()
    line = lax.broadcasted_iota(jnp.int32, (TAIL, tb), 0)
    lane = lax.broadcasted_iota(jnp.int32, (TAIL, tb), 1)
    numbers = [held[row].astype(jnp.float32) for row in range(rows)]
    for g, out in enumerate((own, other)):
        tail = jnp.zeros((TAIL, tb), jnp.float32)
        chosen = lax.broadcasted_iota(jnp.int32, (slots, groups), 1) == place[4 + g]
        for row in range(rows):
            of_group = jnp.sum(jnp.where(chosen, numbers[row], 0.0), axis=1, keepdims=True)
            for slot in range(slots):
                number = jnp.broadcast_to(of_group[slot : slot + 1], (TAIL, tb))
                tail = jnp.where(line == row * slots + slot, number, tail)
        out[pl.ds(rows * slots * tb, TAIL), :] = tail.astype(out.dtype)
    tail = jnp.zeros((TAIL, tb), jnp.float32)
    for row in range(rows):
        for g in range(groups):
            for slot in range(slots):
                number = jnp.broadcast_to(numbers[row][slot : slot + 1, g : g + 1], (TAIL, tb))
                tail = jnp.where((line == row) & (lane == g * slots + slot), number, tail)
    left_tail[...] = tail.astype(left_tail.dtype)
    for copy in copies:
        copy.wait()


def left_payloads(n_y, place, tiles, left_tail, *outs):
    rows, groups, slots, tb, _ = tiles.shape
    per_y = groups // n_y
    for step, out in enumerate(outs):
        to_y = lax.rem(place[1] + step, n_y)
        for row in range(rows):
            for g in range(per_y):
                for slot in range(slots):
                    at = ((row * per_y + g) * slots + slot) * tb
                    out[pl.ds(at, tb), :] = tiles[row, to_y * per_y + g, slot]
        out[pl.ds(rows * per_y * slots * tb, TAIL), :] = left_tail[...]


def listed_columns(rows, place, *refs):
    left, out = refs[:-1], refs[-1]
    for n in range(4):
        out[pl.ds(len(left) * rows + n, 1), :] = jnp.full((1, out.shape[1]), place[n], jnp.int32)
    for n, ref in enumerate(left):
        tail = ref[pl.ds(ref.shape[0] - TAIL, TAIL), :].astype(jnp.float32).astype(jnp.int32)
        out[pl.ds(n * rows, rows), :] = tail[:rows]


def products(n_left, sizes, columns_in, *refs):
    left, right_in = refs[:n_left], refs[n_left:-5]
    out, right, right_columns, columns, listed = refs[-5:]
    fetch = pltpu.make_async_copy(columns_in, columns, listed)
    fetch.start()
    tiles_end = right.shape[1]
    for n, ref in enumerate(right_in[:-2]):
        right[n] = ref[pl.ds(0, tiles_end), :]
        right_columns[pl.ds(n * TAIL, TAIL), :] = ref[pl.ds(tiles_end, TAIL), :].astype(jnp.float32)
    n, (top, bottom), cut = len(right_in) - 2, right_in[-2:], tiles_end // 2
    right[n, pl.ds(0, cut), :] = top[...]
    right[n, pl.ds(cut, cut), :] = bottom[pl.ds(0, cut), :]
    right_columns[pl.ds(n * TAIL, TAIL), :] = bottom[pl.ds(cut, TAIL), :].astype(jnp.float32)
    fetch.wait()
    work = Rows(sizes, columns)
    tb = work.tb
    quarters, quarter = out.shape[1], out.shape[4]
    for n, row in work.all():
        rounded = work.product(left, right, right_columns, n, row).astype(out.dtype)
        for t in range(work.slots):
            for q in range(quarters):
                out[work.place(n), q, row, t] = rounded[
                    q * quarter : (q + 1) * quarter, t * tb : (t + 1) * tb
                ]


def final_sum(n_y, arrived, out):
    rows, groups, slots = out.shape[:3]
    for g in range(groups):
        x, core = divmod(g, 2)
        for row in range(rows):
            for t in range(slots):
                total = arrived[0, core, x, row, t].astype(jnp.float32)
                for y in range(1, n_y):
                    total += arrived[y, core, x, row, t].astype(jnp.float32)
                out[row, g, t] = total.astype(out.dtype)


def on_device(density_tiles, tile_columns):
    rows, groups, slots, tb, _ = density_tiles.shape
    n_x, n_y, n_lo, n_hi = (lax.axis_size(a) for a in ("x", "y", "z_lo", "z_hi"))
    n_z = n_lo * n_hi
    x, y, core = lax.axis_index("x"), lax.axis_index("y"), lax.axis_index("core")
    z = lax.axis_index("z_hi") * n_lo + lax.axis_index("z_lo")
    cores = [(0, 1), (1, 0)]

    smem, vmem = pl.BlockSpec(memory_space=pltpu.SMEM), pl.BlockSpec(memory_space=pltpu.VMEM)
    hbm = pl.BlockSpec(memory_space=pltpu.HBM)
    limit = pltpu.CompilerParams(vmem_limit_bytes=4 * 2**20)
    payload = (rows * slots * tb + TAIL, tb)
    place = jnp.zeros((6,), jnp.int32)
    for n, number in enumerate((x, y, z, core, 2 * x + core, 2 * x + 1 - core)):
        place = jnp.where(lax.iota(jnp.int32, 6) == n, number, place)
    own, other, left_tail = pl.pallas_call(
        first_payloads,
        out_shape=[pltpu.VMEM(shape, jnp.bfloat16) for shape in (payload, payload, (TAIL, tb))],
        in_specs=[smem, hbm, hbm],
        out_specs=[vmem] * 3,
        scratch_shapes=[pltpu.VMEM((rows, slots, groups), jnp.int32), pltpu.SemaphoreType.DMA, pltpu.SemaphoreType.DMA],
        compiler_params=limit,
    )(
        place,
        pltpu.with_memory_space_constraint(tile_columns.transpose(0, 2, 1), pltpu.HBM),
        pltpu.with_memory_space_constraint(density_tiles, pltpu.HBM),
    )
    right = {(0, 0, 0): own}
    held = {(flip, chain): (own, other)[flip] for flip in range(2) for chain in range(2)}

    def ring(step, keys):
        for flip, chain in keys:
            perm = z_pairs((chain + step - 1) % 2, flip if step == 1 else 0, n_hi, n_lo)
            held[flip, chain] = lax.ppermute(held[flip, chain], ZC, perm)
            right[flip, step, chain] = held[flip, chain]

    half = n_z // 2
    every = [(flip, chain) for flip in range(2) for chain in range(2)]
    ring(1, every)

    left_payload = (rows * groups // n_y * slots * tb + TAIL, tb)
    sent = pl.pallas_call(
        functools.partial(left_payloads, n_y),
        out_shape=[pltpu.VMEM(left_payload, jnp.bfloat16)] * n_y,
        in_specs=[smem, vmem, vmem],
        out_specs=[vmem] * n_y,
        compiler_params=limit,
    )(place, *[pltpu.with_memory_space_constraint(a, pltpu.VMEM) for a in (density_tiles, left_tail)])
    left = {(0, 0): sent[0]}
    for step in (2, 1, 3):
        perm = [(s, (s + step) % n_y) for s in range(n_y)]
        left[0, -step % n_y] = lax.ppermute(sent[step], "y", perm)
    right[1, 0, 0] = lax.ppermute(other, "core", cores)
    left[1, 0] = lax.ppermute(left[0, 0], "core", cores)
    for step in range(1, n_y):
        left[1, step] = lax.ppermute(left[0, step], "core", cores)

    for step in range(2, half):
        ring(step, every)
    ring(half, [(0, 0)])
    cut = rows * slots * tb // 2
    far = []
    parts = held[1, 0][:cut], held[1, 1][cut:]
    for chain, part in enumerate(parts):
        far.append(lax.ppermute(part, ZC, z_pairs((chain + half - 1) % 2, 0, n_hi, n_lo)))

    left_keys = [(flip, step) for flip in range(2) for step in range(n_y)]
    sizes = (rows, slots, n_y, n_lo, n_hi, tb)
    quarter = tb // n_x

    rights = [
        right[key]
        for flip in range(2)
        for key in [(flip, 0, 0)]
        + [(flip, step, chain) for step in range(1, half) for chain in range(2)]
        + ([(flip, half, flip)] if flip == 0 else [])
    ] + far
    lefts = [pltpu.with_memory_space_constraint(left[k], pltpu.VMEM) for k in left_keys]
    rights = [pltpu.with_memory_space_constraint(r, pltpu.VMEM) for r in rights]
    columns = pl.pallas_call(
        functools.partial(listed_columns, rows),
        out_shape=pltpu.VMEM((2 * n_y * rows + 8, tb), jnp.int32),
        in_specs=[smem] + [vmem] * len(lefts),
        out_specs=vmem,
        compiler_params=limit,
    )(place, *lefts)
    partial = pl.pallas_call(
        functools.partial(products, len(lefts), sizes),
        out_shape=pltpu.VMEM((2 * n_y, n_x, rows, slots, quarter, tb), jnp.bfloat16),
        in_specs=[vmem] * (1 + len(lefts) + len(rights)),
        out_specs=vmem,
        scratch_shapes=[
            pltpu.VMEM((2 * n_z, payload[0] - TAIL, tb), jnp.bfloat16),
            pltpu.VMEM((2 * n_z * TAIL, tb), jnp.float32),
            pltpu.SMEM((2 * n_y * rows + 8, tb), jnp.int32),
            pltpu.SemaphoreType.DMA,
        ],
        compiler_params=pltpu.CompilerParams(vmem_limit_bytes=12 * 2**20),
    )(pltpu.with_memory_space_constraint(columns, pltpu.VMEM), *lefts, *rights)

    arrived = lax.all_to_all(
        partial.reshape(2 * n_y * n_x, rows, slots, quarter, tb),
        ("y", "core", "x"),
        split_axis=0,
        concat_axis=0,
        tiled=True,
    )
    arrived = arrived.reshape(n_y, 2, n_x, rows, slots, quarter, tb)
    return pl.pallas_call(
        functools.partial(final_sum, n_y),
        out_shape=jax.ShapeDtypeStruct((rows, groups, slots, quarter, tb), jnp.bfloat16),
        in_specs=[vmem],
        out_specs=vmem,
        compiler_params=limit,
    )(pltpu.with_memory_space_constraint(arrived, pltpu.VMEM))


def solution(mesh):
    fine = Mesh(mesh.devices.reshape(4, 2, 4, 2, 4), ("y", "z_lo", "z_hi", "core", "x"))

    return jax.shard_map(
        on_device,
        mesh=fine,
        in_specs=(P(ROWS_COLS, None, None, None, None), P(ROWS_COLS, None, None)),
        out_specs=P(ROWS_COLS, None, None, "x", None),
        check_vma=False,
    )
```

```python
import functools

import jax
import jax.numpy as jnp
from jax import lax
from jax.experimental import pallas as pl
from jax.experimental.pallas import tpu as pltpu
from jax.sharding import Mesh
from jax.sharding import PartitionSpec as P


ROWS_COLS = ("y", "z_lo", "z_hi", "core")
ZC = ("z_lo", "z_hi", "core")
TAIL = 8
NO_TARGET = -3


def z_place(z, n_hi, n_lo):
    z = z % (n_hi * n_lo)
    return (z % n_lo) * n_hi + z // n_lo


def z_pairs(odd, flip, n_hi, n_lo):
    n = n_hi * n_lo
    pairs = []
    for z in range(n):
        to = z + 1 if (z + odd) % 2 == 0 else z - 1
        pairs += [
            (z_place(z, n_hi, n_lo) * 2 + c, z_place(to, n_hi, n_lo) * 2 + (c ^ flip)) for c in range(2)
        ]
    return pairs


def picked(tiles, columns, wanted):
    out = []
    for number in wanted:
        total = None
        for tile, column in zip(tiles, columns):
            part = tile * jnp.where(column == number, 1.0, 0.0).astype(tile.dtype)
            total = part if total is None else total + part
        out.append(total)
    return jnp.concatenate(out, axis=1)


class Rows:
    def __init__(self, sizes, columns):
        self.rows, self.slots, self.n_y, self.n_lo, self.n_hi, self.tb = sizes
        self.columns = columns
        self.x, self.y, self.core = (lax.axis_index(axis) for axis in ("x", "y", "core"))
        self.z = lax.axis_index("z_hi") * self.n_lo + lax.axis_index("z_lo")

    def all(self):
        return [(n, row) for n in range(2 * self.n_y) for row in range(self.rows)]

    def place(self, n):
        flip, step = divmod(n, self.n_y)
        return lax.rem(self.y + step, self.n_y) * 2 + (self.core ^ flip)

    def wanted(self, n, row):
        at = (2 * self.x + self.core) * self.slots
        return [self.columns[n * self.rows + row, at + t] for t in range(self.slots)]

    def inner(self, n, row, group, slot):
        n_z = self.n_lo * self.n_hi
        first = self.n_lo * self.y + group
        column = self.columns[n * self.rows + row, first * self.slots + slot]
        listed = column >= 0
        local = jnp.where(listed, column - first * (self.rows * 2 * self.n_hi), 0)
        owner = lax.div(local, self.rows)
        inner_z = lax.div(owner, 2) * self.n_lo + group
        ahead = lax.rem(inner_z - self.z + n_z, n_z)
        steps = jnp.minimum(ahead, n_z - ahead)
        chain = lax.rem(self.z + steps + jnp.where(ahead < n_z // 2, 1, 0), 2)
        at = jnp.where(ahead == 0, 0, jnp.where(ahead == n_z // 2, n_z - 1, 2 * steps - 1 + chain))
        source = (lax.rem(owner, 2) ^ self.core) * n_z + at
        return listed, source, (local - owner * self.rows) * self.slots

    def product(self, left, right, right_columns, n, row):
        tb, slots = self.tb, self.slots
        wanted = self.wanted(n, row)
        total = None
        for group in range(self.n_lo):
            lefts, rights = [], []
            for slot in range(slots):
                here, source, at = self.inner(n, row, group, slot)
                tiles = [
                    right[source, pl.ds(pl.multiple_of((at + s) * tb, tb), tb), :]
                    for s in range(slots)
                ]
                listed = [right_columns[pl.ds(source * TAIL + at + s, 1), :] for s in range(slots)]
                numbers = [
                    jnp.where(here & (wanted[t] >= 0), wanted[t], NO_TARGET).astype(jnp.float32)
                    for t in range(slots)
                ]
                rows = pl.ds(((row * self.n_lo + group) * slots + slot) * tb, tb)
                lefts.append(left[n][rows, :])
                rights.append(picked(tiles, listed, numbers))
            part = jnp.dot(
                jnp.concatenate(lefts, axis=1),
                jnp.concatenate(rights, axis=0),
                preferred_element_type=jnp.float32,
            )
            total = part if total is None else total + part
        return total


def first_payloads(columns, tiles, own, other, left_tail, held, arrived, listed):
    rows, groups, slots, tb, _ = tiles.shape
    x, core = lax.axis_index("x"), lax.axis_index("core")
    chosen_groups = (2 * x + core, 2 * x + 1 - core)
    copies = [
        pltpu.make_async_copy(tiles.at[row, chosen_groups[g], slot], out.at[pl.ds((row * slots + slot) * tb, tb)], arrived)
        for g, out in enumerate((own, other))
        for row in range(rows)
        for slot in range(slots)
    ]
    fetch = pltpu.make_async_copy(columns, held, listed)
    fetch.start()
    for copy in copies:
        copy.start()
    fetch.wait()
    line = lax.broadcasted_iota(jnp.int32, (TAIL, tb), 0)
    lane = lax.broadcasted_iota(jnp.int32, (TAIL, tb), 1)
    numbers = [held[row].astype(jnp.float32) for row in range(rows)]
    for g, out in enumerate((own, other)):
        tail = jnp.zeros((TAIL, tb), jnp.float32)
        chosen = lax.broadcasted_iota(jnp.int32, (slots, groups), 1) == chosen_groups[g]
        for row in range(rows):
            of_group = jnp.sum(jnp.where(chosen, numbers[row], 0.0), axis=1, keepdims=True)
            for slot in range(slots):
                number = jnp.broadcast_to(of_group[slot : slot + 1], (TAIL, tb))
                tail = jnp.where(line == row * slots + slot, number, tail)
        out[pl.ds(rows * slots * tb, TAIL), :] = tail.astype(out.dtype)
    tail = jnp.zeros((TAIL, tb), jnp.float32)
    for row in range(rows):
        for g in range(groups):
            for slot in range(slots):
                number = jnp.broadcast_to(numbers[row][slot : slot + 1, g : g + 1], (TAIL, tb))
                tail = jnp.where((line == row) & (lane == g * slots + slot), number, tail)
    left_tail[...] = tail.astype(left_tail.dtype)
    for copy in copies:
        copy.wait()


def left_payloads(n_y, tiles, left_tail, *outs):
    rows, groups, slots, tb, _ = tiles.shape
    per_y = groups // n_y
    for step, out in enumerate(outs):
        to_y = lax.rem(lax.axis_index("y") + step, n_y)
        for row in range(rows):
            for g in range(per_y):
                for slot in range(slots):
                    at = ((row * per_y + g) * slots + slot) * tb
                    out[pl.ds(at, tb), :] = tiles[row, to_y * per_y + g, slot]
        out[pl.ds(rows * per_y * slots * tb, TAIL), :] = left_tail[...]


def listed_columns(rows, *refs):
    left, out = refs[:-1], refs[-1]
    for n, ref in enumerate(left):
        tail = ref[pl.ds(ref.shape[0] - TAIL, TAIL), :].astype(jnp.float32).astype(jnp.int32)
        out[pl.ds(n * rows, rows), :] = tail[:rows]


def products(n_left, sizes, columns_in, *refs):
    left, right_in = refs[:n_left], refs[n_left:-5]
    out, right, right_columns, columns, listed = refs[-5:]
    fetch = pltpu.make_async_copy(columns_in, columns, listed)
    fetch.start()
    tiles_end = right.shape[1]
    for n, ref in enumerate(right_in):
        right[n] = ref[pl.ds(0, tiles_end), :]
        right_columns[pl.ds(n * TAIL, TAIL), :] = ref[pl.ds(tiles_end, TAIL), :].astype(jnp.float32)
    fetch.wait()
    work = Rows(sizes, columns)
    tb = work.tb
    quarters, quarter = out.shape[1], out.shape[4]
    for n, row in work.all():
        rounded = work.product(left, right, right_columns, n, row).astype(out.dtype)
        for t in range(work.slots):
            for q in range(quarters):
                out[work.place(n), q, row, t] = rounded[
                    q * quarter : (q + 1) * quarter, t * tb : (t + 1) * tb
                ]


def final_sum(n_y, arrived, out):
    rows, groups, slots = out.shape[:3]
    for g in range(groups):
        x, core = divmod(g, 2)
        for row in range(rows):
            for t in range(slots):
                total = arrived[0, core, x, row, t].astype(jnp.float32)
                for y in range(1, n_y):
                    total += arrived[y, core, x, row, t].astype(jnp.float32)
                out[row, g, t] = total.astype(out.dtype)


def on_device(density_tiles, tile_columns):
    rows, groups, slots, tb, _ = density_tiles.shape
    n_x, n_y, n_lo, n_hi = (lax.axis_size(a) for a in ("x", "y", "z_lo", "z_hi"))
    n_z = n_lo * n_hi
    cores = [(0, 1), (1, 0)]

    vmem = pl.BlockSpec(memory_space=pltpu.VMEM)
    hbm = pl.BlockSpec(memory_space=pltpu.HBM)
    limit = pltpu.CompilerParams(vmem_limit_bytes=4 * 2**20)
    payload = (rows * slots * tb + TAIL, tb)
    own, other, left_tail = pl.pallas_call(
        first_payloads,
        out_shape=[pltpu.VMEM(shape, jnp.bfloat16) for shape in (payload, payload, (TAIL, tb))],
        in_specs=[hbm, hbm],
        out_specs=[vmem] * 3,
        scratch_shapes=[
            pltpu.VMEM((rows, slots, groups), jnp.int32),
            pltpu.SemaphoreType.DMA,
            pltpu.SemaphoreType.DMA,
        ],
        compiler_params=limit,
    )(
        pltpu.with_memory_space_constraint(tile_columns.transpose(0, 2, 1), pltpu.HBM),
        pltpu.with_memory_space_constraint(density_tiles, pltpu.HBM),
    )
    right = {(0, 0, 0): own}
    held = {(flip, chain): (own, other)[flip] for flip in range(2) for chain in range(2)}

    def ring(step, keys):
        for flip, chain in keys:
            perm = z_pairs((chain + step - 1) % 2, flip if step == 1 else 0, n_hi, n_lo)
            held[flip, chain] = lax.ppermute(held[flip, chain], ZC, perm)
            right[flip, step, chain] = held[flip, chain]

    half = n_z // 2
    every = [(flip, chain) for flip in range(2) for chain in range(2)]
    ring(1, every)

    left_payload = (rows * groups // n_y * slots * tb + TAIL, tb)
    sent = pl.pallas_call(
        functools.partial(left_payloads, n_y),
        out_shape=[pltpu.VMEM(left_payload, jnp.bfloat16)] * n_y,
        in_specs=[vmem, vmem],
        out_specs=[vmem] * n_y,
        compiler_params=limit,
    )(*[pltpu.with_memory_space_constraint(a, pltpu.VMEM) for a in (density_tiles, left_tail)])
    left = {(0, 0): sent[0]}
    for step in (2, 1, 3):
        perm = [(s, (s + step) % n_y) for s in range(n_y)]
        left[0, -step % n_y] = lax.ppermute(sent[step], "y", perm)
    right[1, 0, 0] = lax.ppermute(other, "core", cores)
    left[1, 0] = lax.ppermute(left[0, 0], "core", cores)
    for step in range(1, n_y):
        left[1, step] = lax.ppermute(left[0, step], "core", cores)

    for step in range(2, half):
        ring(step, every)
    ring(half, [(0, 0), (1, 1)])

    left_keys = [(flip, step) for flip in range(2) for step in range(n_y)]
    sizes = (rows, slots, n_y, n_lo, n_hi, tb)
    quarter = tb // n_x

    rights = [
        right[key]
        for flip in range(2)
        for key in [(flip, 0, 0)]
        + [(flip, step, chain) for step in range(1, half) for chain in range(2)]
        + [(flip, half, flip)]
    ]
    lefts = [pltpu.with_memory_space_constraint(left[k], pltpu.VMEM) for k in left_keys]
    rights = [pltpu.with_memory_space_constraint(r, pltpu.VMEM) for r in rights]
    columns = pl.pallas_call(
        functools.partial(listed_columns, rows),
        out_shape=pltpu.VMEM((2 * n_y * rows, tb), jnp.int32),
        in_specs=[vmem] * len(lefts),
        out_specs=vmem,
        compiler_params=limit,
    )(*lefts)
    partial = pl.pallas_call(
        functools.partial(products, len(lefts), sizes),
        out_shape=pltpu.VMEM((2 * n_y, n_x, rows, slots, quarter, tb), jnp.bfloat16),
        in_specs=[vmem] * (1 + len(lefts) + len(rights)),
        out_specs=vmem,
        scratch_shapes=[
            pltpu.VMEM((len(rights), payload[0] - TAIL, tb), jnp.bfloat16),
            pltpu.VMEM((len(rights) * TAIL, tb), jnp.float32),
            pltpu.SMEM((2 * n_y * rows, tb), jnp.int32),
            pltpu.SemaphoreType.DMA,
        ],
        compiler_params=pltpu.CompilerParams(vmem_limit_bytes=12 * 2**20),
    )(pltpu.with_memory_space_constraint(columns, pltpu.VMEM), *lefts, *rights)

    arrived = lax.all_to_all(
        partial.reshape(2 * n_y * n_x, rows, slots, quarter, tb),
        ("y", "core", "x"),
        split_axis=0,
        concat_axis=0,
        tiled=True,
    )
    arrived = arrived.reshape(n_y, 2, n_x, rows, slots, quarter, tb)
    return pl.pallas_call(
        functools.partial(final_sum, n_y),
        out_shape=jax.ShapeDtypeStruct((rows, groups, slots, quarter, tb), jnp.bfloat16),
        in_specs=[vmem],
        out_specs=vmem,
        compiler_params=limit,
    )(pltpu.with_memory_space_constraint(arrived, pltpu.VMEM))


def solution(mesh):
    fine = Mesh(mesh.devices.reshape(4, 2, 4, 2, 4), ("y", "z_lo", "z_hi", "core", "x"))

    return jax.shard_map(
        on_device,
        mesh=fine,
        in_specs=(P(ROWS_COLS, None, None, None, None), P(ROWS_COLS, None, None)),
        out_specs=P(ROWS_COLS, None, None, "x", None),
        check_vma=False,
    )
```

```python
import functools

import jax
import jax.numpy as jnp
from jax import lax
from jax.experimental import pallas as pl
from jax.experimental.pallas import tpu as pltpu
from jax.sharding import Mesh
from jax.sharding import PartitionSpec as P


ROWS_COLS = ("y", "z_lo", "z_hi", "core")
ZC = ("z_lo", "z_hi", "core")
TAIL = 8
NO_TARGET = -3


def z_place(z, n_hi, n_lo):
    z = z % (n_hi * n_lo)
    return (z % n_lo) * n_hi + z // n_lo


def z_pairs(odd, flip, n_hi, n_lo):
    n = n_hi * n_lo
    pairs = []
    for z in range(n):
        to = z + 1 if (z + odd) % 2 == 0 else z - 1
        pairs += [
            (z_place(z, n_hi, n_lo) * 2 + c, z_place(to, n_hi, n_lo) * 2 + (c ^ flip)) for c in range(2)
        ]
    return pairs


def picked(tiles, columns, wanted):
    out = []
    for number in wanted:
        total = None
        for tile, column in zip(tiles, columns):
            part = tile * jnp.where(column == number, 1.0, 0.0).astype(tile.dtype)
            total = part if total is None else total + part
        out.append(total)
    return jnp.concatenate(out, axis=1)


class Rows:
    def __init__(self, sizes, columns):
        self.rows, self.slots, self.n_y, self.n_lo, self.n_hi, self.tb = sizes
        self.columns = columns
        self.x, self.y, self.core = (lax.axis_index(axis) for axis in ("x", "y", "core"))
        self.z = lax.axis_index("z_hi") * self.n_lo + lax.axis_index("z_lo")

    def all(self):
        return [(n, row) for n in range(2 * self.n_y) for row in range(self.rows)]

    def place(self, n):
        flip, step = divmod(n, self.n_y)
        return lax.rem(self.y + step, self.n_y) * 2 + (self.core ^ flip)

    def wanted(self, n, row):
        at = (2 * self.x + self.core) * self.slots
        return [self.columns[n * self.rows + row, at + t] for t in range(self.slots)]

    def inner(self, n, row, group, slot):
        n_z = self.n_lo * self.n_hi
        first = self.n_lo * self.y + group
        column = self.columns[n * self.rows + row, first * self.slots + slot]
        listed = column >= 0
        local = jnp.where(listed, column - first * (self.rows * 2 * self.n_hi), 0)
        owner = lax.div(local, self.rows)
        inner_z = lax.div(owner, 2) * self.n_lo + group
        ahead = lax.rem(inner_z - self.z + n_z, n_z)
        steps = jnp.minimum(ahead, n_z - ahead)
        chain = lax.rem(self.z + steps + jnp.where(ahead < n_z // 2, 1, 0), 2)
        at = jnp.where(ahead == 0, 0, jnp.where(ahead == n_z // 2, n_z - 1, 2 * steps - 1 + chain))
        source = (lax.rem(owner, 2) ^ self.core) * n_z + at
        return listed, source, (local - owner * self.rows) * self.slots

    def product(self, left, right, right_columns, n, row):
        tb, slots = self.tb, self.slots
        wanted = self.wanted(n, row)
        total = None
        for group in range(self.n_lo):
            lefts, rights = [], []
            for slot in range(slots):
                here, source, at = self.inner(n, row, group, slot)
                tiles = [
                    right[source, pl.ds(pl.multiple_of((at + s) * tb, tb), tb), :]
                    for s in range(slots)
                ]
                listed = [right_columns[pl.ds(source * TAIL + at + s, 1), :] for s in range(slots)]
                numbers = [
                    jnp.where(here & (wanted[t] >= 0), wanted[t], NO_TARGET).astype(jnp.float32)
                    for t in range(slots)
                ]
                rows = pl.ds(((row * self.n_lo + group) * slots + slot) * tb, tb)
                lefts.append(left[n][rows, :])
                rights.append(picked(tiles, listed, numbers))
            part = jnp.dot(
                jnp.concatenate(lefts, axis=1),
                jnp.concatenate(rights, axis=0),
                preferred_element_type=jnp.float32,
            )
            total = part if total is None else total + part
        return total


def first_payloads(columns, tiles, own, other, left_tail, held, arrived, listed):
    rows, groups, slots, tb, _ = tiles.shape
    x, core = lax.axis_index("x"), lax.axis_index("core")
    chosen_groups = (2 * x + core, 2 * x + 1 - core)
    copies = [
        pltpu.make_async_copy(tiles.at[row, chosen_groups[g], slot], out.at[pl.ds((row * slots + slot) * tb, tb)], arrived)
        for g, out in enumerate((own, other))
        for row in range(rows)
        for slot in range(slots)
    ]
    fetch = pltpu.make_async_copy(columns, held, listed)
    fetch.start()
    for copy in copies:
        copy.start()
    fetch.wait()
    line = lax.broadcasted_iota(jnp.int32, (TAIL, tb), 0)
    lane = lax.broadcasted_iota(jnp.int32, (TAIL, tb), 1)
    numbers = [held[row].astype(jnp.float32) for row in range(rows)]
    for g, out in enumerate((own, other)):
        tail = jnp.zeros((TAIL, tb), jnp.float32)
        chosen = lax.broadcasted_iota(jnp.int32, (slots, groups), 1) == chosen_groups[g]
        for row in range(rows):
            of_group = jnp.sum(jnp.where(chosen, numbers[row], 0.0), axis=1, keepdims=True)
            for slot in range(slots):
                number = jnp.broadcast_to(of_group[slot : slot + 1], (TAIL, tb))
                tail = jnp.where(line == row * slots + slot, number, tail)
        out[pl.ds(rows * slots * tb, TAIL), :] = tail.astype(out.dtype)
    tail = jnp.zeros((TAIL, tb), jnp.float32)
    for row in range(rows):
        for g in range(groups):
            for slot in range(slots):
                number = jnp.broadcast_to(numbers[row][slot : slot + 1, g : g + 1], (TAIL, tb))
                tail = jnp.where((line == row) & (lane == g * slots + slot), number, tail)
    left_tail[...] = tail.astype(left_tail.dtype)
    for copy in copies:
        copy.wait()


def left_payloads(n_y, tiles, left_tail, *outs):
    rows, groups, slots, tb, _ = tiles.shape
    per_y = groups // n_y
    for step, out in enumerate(outs):
        to_y = lax.rem(lax.axis_index("y") + step, n_y)
        for row in range(rows):
            for g in range(per_y):
                for slot in range(slots):
                    at = ((row * per_y + g) * slots + slot) * tb
                    out[pl.ds(at, tb), :] = tiles[row, to_y * per_y + g, slot]
        out[pl.ds(rows * per_y * slots * tb, TAIL), :] = left_tail[...]


def hold(right, right_columns, n, payload):
    tiles_end = right.shape[1]
    right[n] = payload[pl.ds(0, tiles_end), :]
    right_columns[pl.ds(n * TAIL, TAIL), :] = payload[pl.ds(tiles_end, TAIL), :].astype(jnp.float32)


def hold_early(rows, n_left, *refs):
    left, right_in, (columns, right, right_columns) = refs[:n_left], refs[n_left:-3], refs[-3:]
    for n, ref in enumerate(left):
        tail = ref[pl.ds(ref.shape[0] - TAIL, TAIL), :].astype(jnp.float32).astype(jnp.int32)
        columns[pl.ds(n * rows, rows), :] = tail[:rows]
    per_core = len(right_in) // 2
    for n, ref in enumerate(right_in):
        hold(right, right_columns, n + n // per_core, ref)


def products(n_left, sizes, columns, *refs):
    left, last = refs[:n_left], refs[n_left : n_left + 2]
    out, right, right_columns = refs[-3:]
    for flip, ref in enumerate(last):
        hold(right, right_columns, (flip + 1) * right.shape[0] // 2 - 1, ref)
    work = Rows(sizes, columns)
    tb = work.tb
    quarters, quarter = out.shape[1], out.shape[4]
    for n, row in work.all():
        rounded = work.product(left, right, right_columns, n, row).astype(out.dtype)
        for t in range(work.slots):
            for q in range(quarters):
                out[work.place(n), q, row, t] = rounded[
                    q * quarter : (q + 1) * quarter, t * tb : (t + 1) * tb
                ]


def final_sum(n_y, arrived, out):
    rows, groups, slots = out.shape[:3]
    for g in range(groups):
        x, core = divmod(g, 2)
        for row in range(rows):
            for t in range(slots):
                total = arrived[0, core, x, row, t].astype(jnp.float32)
                for y in range(1, n_y):
                    total += arrived[y, core, x, row, t].astype(jnp.float32)
                out[row, g, t] = total.astype(out.dtype)


def on_device(density_tiles, tile_columns):
    rows, groups, slots, tb, _ = density_tiles.shape
    n_x, n_y, n_lo, n_hi = (lax.axis_size(a) for a in ("x", "y", "z_lo", "z_hi"))
    n_z = n_lo * n_hi
    cores = [(0, 1), (1, 0)]

    vmem = pl.BlockSpec(memory_space=pltpu.VMEM)
    hbm = pl.BlockSpec(memory_space=pltpu.HBM)
    limit = pltpu.CompilerParams(vmem_limit_bytes=4 * 2**20)
    payload = (rows * slots * tb + TAIL, tb)
    own, other, left_tail = pl.pallas_call(
        first_payloads,
        out_shape=[pltpu.VMEM(shape, jnp.bfloat16) for shape in (payload, payload, (TAIL, tb))],
        in_specs=[hbm, hbm],
        out_specs=[vmem] * 3,
        scratch_shapes=[pltpu.VMEM((rows, slots, groups), jnp.int32), pltpu.SemaphoreType.DMA, pltpu.SemaphoreType.DMA],
        compiler_params=limit,
    )(
        pltpu.with_memory_space_constraint(tile_columns.transpose(0, 2, 1), pltpu.HBM),
        pltpu.with_memory_space_constraint(density_tiles, pltpu.HBM),
    )
    right = {(0, 0, 0): own}
    held = {(flip, chain): (own, other)[flip] for flip in range(2) for chain in range(2)}

    def ring(step, keys):
        for flip, chain in keys:
            perm = z_pairs((chain + step - 1) % 2, flip if step == 1 else 0, n_hi, n_lo)
            held[flip, chain] = lax.ppermute(held[flip, chain], ZC, perm)
            right[flip, step, chain] = held[flip, chain]

    half = n_z // 2
    every = [(flip, chain) for flip in range(2) for chain in range(2)]
    ring(1, every)

    left_payload = (rows * groups // n_y * slots * tb + TAIL, tb)
    sent = pl.pallas_call(
        functools.partial(left_payloads, n_y),
        out_shape=[pltpu.VMEM(left_payload, jnp.bfloat16)] * n_y,
        in_specs=[vmem, vmem],
        out_specs=[vmem] * n_y,
        compiler_params=limit,
    )(*[pltpu.with_memory_space_constraint(a, pltpu.VMEM) for a in (density_tiles, left_tail)])
    left = {(0, 0): sent[0]}
    for step in (2, 1, 3):
        perm = [(s, (s + step) % n_y) for s in range(n_y)]
        left[0, -step % n_y] = lax.ppermute(sent[step], "y", perm)
    right[1, 0, 0] = lax.ppermute(other, "core", cores)
    left[1, 0] = lax.ppermute(left[0, 0], "core", cores)
    for step in range(1, n_y):
        left[1, step] = lax.ppermute(left[0, step], "core", cores)

    for step in range(2, half):
        ring(step, every)
    ring(half, [(0, 0), (1, 1)])

    left_keys = [(flip, step) for flip in range(2) for step in range(n_y)]
    sizes = (rows, slots, n_y, n_lo, n_hi, tb)
    quarter = tb // n_x

    rights = [
        right[key]
        for flip in range(2)
        for key in [(flip, 0, 0)]
        + [(flip, step, chain) for step in range(1, half) for chain in range(2)]
        + [(flip, half, flip)]
    ]
    lefts = [pltpu.with_memory_space_constraint(left[k], pltpu.VMEM) for k in left_keys]
    rights = [pltpu.with_memory_space_constraint(r, pltpu.VMEM) for r in rights]
    early, last = rights[: n_z - 1] + rights[n_z:-1], [rights[n_z - 1], rights[-1]]
    held_shapes = [
        pltpu.VMEM((2 * n_z, payload[0] - TAIL, tb), jnp.bfloat16),
        pltpu.VMEM((2 * n_z * TAIL, tb), jnp.float32),
    ]
    columns, *kept = pl.pallas_call(
        functools.partial(hold_early, rows, len(lefts)),
        out_shape=[jax.ShapeDtypeStruct((2 * n_y * rows, tb), jnp.int32)] + held_shapes,
        in_specs=[vmem] * (len(lefts) + len(early)),
        out_specs=[vmem] * 3,
        compiler_params=limit,
    )(*lefts, *early)
    kept = [pltpu.with_memory_space_constraint(k, pltpu.VMEM) for k in kept]
    operands = [pltpu.with_memory_space_constraint(columns, pltpu.SMEM), *lefts, *last, *kept]
    partial, _, _ = pl.pallas_call(
        functools.partial(products, len(lefts), sizes),
        out_shape=[pltpu.VMEM((2 * n_y, n_x, rows, slots, quarter, tb), jnp.bfloat16)] + held_shapes,
        in_specs=[pl.BlockSpec(memory_space=pltpu.SMEM)] + [vmem] * (len(operands) - 1),
        out_specs=[vmem] * 3,
        input_output_aliases={len(operands) - 2: 1, len(operands) - 1: 2},
        compiler_params=limit,
    )(*operands)

    arrived = lax.all_to_all(
        partial.reshape(2 * n_y * n_x, rows, slots, quarter, tb),
        ("y", "core", "x"),
        split_axis=0,
        concat_axis=0,
        tiled=True,
    )
    arrived = arrived.reshape(n_y, 2, n_x, rows, slots, quarter, tb)
    return pl.pallas_call(
        functools.partial(final_sum, n_y),
        out_shape=jax.ShapeDtypeStruct((rows, groups, slots, quarter, tb), jnp.bfloat16),
        in_specs=[vmem],
        out_specs=vmem,
        compiler_params=limit,
    )(pltpu.with_memory_space_constraint(arrived, pltpu.VMEM))


def solution(mesh):
    fine = Mesh(mesh.devices.reshape(4, 2, 4, 2, 4), ("y", "z_lo", "z_hi", "core", "x"))

    return jax.shard_map(
        on_device,
        mesh=fine,
        in_specs=(P(ROWS_COLS, None, None, None, None), P(ROWS_COLS, None, None)),
        out_specs=P(ROWS_COLS, None, None, "x", None),
        check_vma=False,
    )
```

```python
import functools

import jax
import jax.numpy as jnp
from jax import lax
from jax.experimental import pallas as pl
from jax.experimental.pallas import tpu as pltpu
from jax.sharding import Mesh
from jax.sharding import PartitionSpec as P


ROWS_COLS = ("y", "z_lo", "z_hi", "core")
ZC = ("z_lo", "z_hi", "core")
TAIL = 8
NO_TARGET = -3


def z_place(z, n_hi, n_lo):
    z = z % (n_hi * n_lo)
    return (z % n_lo) * n_hi + z // n_lo


def z_pairs(odd, flip, n_hi, n_lo):
    n = n_hi * n_lo
    pairs = []
    for z in range(n):
        to = z + 1 if (z + odd) % 2 == 0 else z - 1
        pairs += [
            (z_place(z, n_hi, n_lo) * 2 + c, z_place(to, n_hi, n_lo) * 2 + (c ^ flip)) for c in range(2)
        ]
    return pairs


def picked(tiles, columns, wanted):
    out = []
    for number in wanted:
        total = None
        for tile, column in zip(tiles, columns):
            part = tile * jnp.where(column == number, 1.0, 0.0).astype(tile.dtype)
            total = part if total is None else total + part
        out.append(total)
    return jnp.concatenate(out, axis=1)


class Rows:
    def __init__(self, sizes, columns):
        self.rows, self.slots, self.n_y, self.n_lo, self.n_hi, self.tb = sizes
        self.columns = columns
        self.x, self.y, self.core = (lax.axis_index(axis) for axis in ("x", "y", "core"))
        self.z = lax.axis_index("z_hi") * self.n_lo + lax.axis_index("z_lo")

    def all(self):
        return [(n, row) for n in range(2 * self.n_y) for row in range(self.rows)]

    def place(self, n):
        flip, step = divmod(n, self.n_y)
        return lax.rem(self.y + step, self.n_y) * 2 + (self.core ^ flip)

    def wanted(self, n, row):
        at = (2 * self.x + self.core) * self.slots
        return [self.columns[n * self.rows + row, at + t] for t in range(self.slots)]

    def inner(self, n, row, group, slot):
        n_z = self.n_lo * self.n_hi
        first = self.n_lo * self.y + group
        column = self.columns[n * self.rows + row, first * self.slots + slot]
        listed = column >= 0
        local = jnp.where(listed, column - first * (self.rows * 2 * self.n_hi), 0)
        owner = lax.div(local, self.rows)
        inner_z = lax.div(owner, 2) * self.n_lo + group
        ahead = lax.rem(inner_z - self.z + n_z, n_z)
        steps = jnp.minimum(ahead, n_z - ahead)
        chain = lax.rem(self.z + steps + jnp.where(ahead < n_z // 2, 1, 0), 2)
        at = jnp.where(ahead == 0, 0, jnp.where(ahead == n_z // 2, n_z - 1, 2 * steps - 1 + chain))
        source = (lax.rem(owner, 2) ^ self.core) * n_z + at
        return listed, source, (local - owner * self.rows) * self.slots

    def product(self, left, right, right_columns, n, row):
        tb, slots = self.tb, self.slots
        wanted = self.wanted(n, row)
        total = None
        for group in range(self.n_lo):
            lefts, rights = [], []
            for slot in range(slots):
                here, source, at = self.inner(n, row, group, slot)
                tiles = [
                    right[source, pl.ds(pl.multiple_of((at + s) * tb, tb), tb), :]
                    for s in range(slots)
                ]
                listed = [right_columns[pl.ds(source * TAIL + at + s, 1), :] for s in range(slots)]
                numbers = [
                    jnp.where(here & (wanted[t] >= 0), wanted[t], NO_TARGET).astype(jnp.float32)
                    for t in range(slots)
                ]
                rows = pl.ds(((row * self.n_lo + group) * slots + slot) * tb, tb)
                lefts.append(left[n][rows, :])
                rights.append(picked(tiles, listed, numbers))
            part = jnp.dot(
                jnp.concatenate(lefts, axis=1),
                jnp.concatenate(rights, axis=0),
                preferred_element_type=jnp.float32,
            )
            total = part if total is None else total + part
        return total


def first_payloads(columns, tiles, own, other, left_tail, held, arrived, listed):
    rows, groups, slots, tb, _ = tiles.shape
    x, core = lax.axis_index("x"), lax.axis_index("core")
    chosen_groups = (2 * x + core, 2 * x + 1 - core)
    copies = [
        pltpu.make_async_copy(tiles.at[row, chosen_groups[g], slot], out.at[pl.ds((row * slots + slot) * tb, tb)], arrived)
        for g, out in enumerate((own, other))
        for row in range(rows)
        for slot in range(slots)
    ]
    fetch = pltpu.make_async_copy(columns, held, listed)
    fetch.start()
    for copy in copies:
        copy.start()
    fetch.wait()
    line = lax.broadcasted_iota(jnp.int32, (TAIL, tb), 0)
    lane = lax.broadcasted_iota(jnp.int32, (TAIL, tb), 1)
    numbers = [held[row].astype(jnp.float32) for row in range(rows)]
    for g, out in enumerate((own, other)):
        tail = jnp.zeros((TAIL, tb), jnp.float32)
        chosen = lax.broadcasted_iota(jnp.int32, (slots, groups), 1) == chosen_groups[g]
        for row in range(rows):
            of_group = jnp.sum(jnp.where(chosen, numbers[row], 0.0), axis=1, keepdims=True)
            for slot in range(slots):
                number = jnp.broadcast_to(of_group[slot : slot + 1], (TAIL, tb))
                tail = jnp.where(line == row * slots + slot, number, tail)
        out[pl.ds(rows * slots * tb, TAIL), :] = tail.astype(out.dtype)
    tail = jnp.zeros((TAIL, tb), jnp.float32)
    for row in range(rows):
        for g in range(groups):
            for slot in range(slots):
                number = jnp.broadcast_to(numbers[row][slot : slot + 1, g : g + 1], (TAIL, tb))
                tail = jnp.where((line == row) & (lane == g * slots + slot), number, tail)
    left_tail[...] = tail.astype(left_tail.dtype)
    for copy in copies:
        copy.wait()


def left_payloads(n_y, tiles, left_tail, *outs):
    rows, groups, slots, tb, _ = tiles.shape
    per_y = groups // n_y
    for step, out in enumerate(outs):
        to_y = lax.rem(lax.axis_index("y") + step, n_y)
        for row in range(rows):
            for g in range(per_y):
                for slot in range(slots):
                    at = ((row * per_y + g) * slots + slot) * tb
                    out[pl.ds(at, tb), :] = tiles[row, to_y * per_y + g, slot]
        out[pl.ds(rows * per_y * slots * tb, TAIL), :] = left_tail[...]


def hold(right, right_columns, n, payload):
    tiles_end = right.shape[1]
    right[n] = payload[pl.ds(0, tiles_end), :]
    right_columns[pl.ds(n * TAIL, TAIL), :] = payload[pl.ds(tiles_end, TAIL), :].astype(jnp.float32)


def hold_early(rows, n_left, *refs):
    left, right_in = refs[:n_left], refs[n_left:-5]
    columns, right, right_columns, listed, arrived = refs[-5:]
    for n, ref in enumerate(left):
        tail = ref[pl.ds(ref.shape[0] - TAIL, TAIL), :].astype(jnp.float32).astype(jnp.int32)
        listed[pl.ds(n * rows, rows), :] = tail[:rows]
    fetch = pltpu.make_async_copy(listed, columns, arrived)
    fetch.start()
    per_core = len(right_in) // 2
    for n, ref in enumerate(right_in):
        hold(right, right_columns, n + n // per_core, ref)
    fetch.wait()


def products(n_left, sizes, columns, *refs):
    left, last = refs[:n_left], refs[n_left : n_left + 2]
    out, right, right_columns = refs[-3:]
    for flip, ref in enumerate(last):
        hold(right, right_columns, (flip + 1) * right.shape[0] // 2 - 1, ref)
    work = Rows(sizes, columns)
    tb = work.tb
    quarters, quarter = out.shape[1], out.shape[4]
    for n, row in work.all():
        rounded = work.product(left, right, right_columns, n, row).astype(out.dtype)
        for t in range(work.slots):
            for q in range(quarters):
                out[work.place(n), q, row, t] = rounded[
                    q * quarter : (q + 1) * quarter, t * tb : (t + 1) * tb
                ]


def final_sum(n_y, arrived, out):
    rows, groups, slots = out.shape[:3]
    for g in range(groups):
        x, core = divmod(g, 2)
        for row in range(rows):
            for t in range(slots):
                total = arrived[0, core, x, row, t].astype(jnp.float32)
                for y in range(1, n_y):
                    total += arrived[y, core, x, row, t].astype(jnp.float32)
                out[row, g, t] = total.astype(out.dtype)


def on_device(density_tiles, tile_columns):
    rows, groups, slots, tb, _ = density_tiles.shape
    n_x, n_y, n_lo, n_hi = (lax.axis_size(a) for a in ("x", "y", "z_lo", "z_hi"))
    n_z = n_lo * n_hi
    cores = [(0, 1), (1, 0)]

    vmem = pl.BlockSpec(memory_space=pltpu.VMEM)
    hbm = pl.BlockSpec(memory_space=pltpu.HBM)
    limit = pltpu.CompilerParams(vmem_limit_bytes=4 * 2**20)
    payload = (rows * slots * tb + TAIL, tb)
    own, other, left_tail = pl.pallas_call(
        first_payloads,
        out_shape=[pltpu.VMEM(shape, jnp.bfloat16) for shape in (payload, payload, (TAIL, tb))],
        in_specs=[hbm, hbm],
        out_specs=[vmem] * 3,
        scratch_shapes=[pltpu.VMEM((rows, slots, groups), jnp.int32), pltpu.SemaphoreType.DMA, pltpu.SemaphoreType.DMA],
        compiler_params=limit,
    )(
        pltpu.with_memory_space_constraint(tile_columns.transpose(0, 2, 1), pltpu.HBM),
        pltpu.with_memory_space_constraint(density_tiles, pltpu.HBM),
    )
    right = {(0, 0, 0): own}
    held = {(flip, chain): (own, other)[flip] for flip in range(2) for chain in range(2)}

    def ring(step, keys):
        for flip, chain in keys:
            perm = z_pairs((chain + step - 1) % 2, flip if step == 1 else 0, n_hi, n_lo)
            held[flip, chain] = lax.ppermute(held[flip, chain], ZC, perm)
            right[flip, step, chain] = held[flip, chain]

    half = n_z // 2
    every = [(flip, chain) for flip in range(2) for chain in range(2)]
    ring(1, every)

    left_payload = (rows * groups // n_y * slots * tb + TAIL, tb)
    sent = pl.pallas_call(
        functools.partial(left_payloads, n_y),
        out_shape=[pltpu.VMEM(left_payload, jnp.bfloat16)] * n_y,
        in_specs=[vmem, vmem],
        out_specs=[vmem] * n_y,
        compiler_params=limit,
    )(*[pltpu.with_memory_space_constraint(a, pltpu.VMEM) for a in (density_tiles, left_tail)])
    left = {(0, 0): sent[0]}
    for step in (2, 1, 3):
        perm = [(s, (s + step) % n_y) for s in range(n_y)]
        left[0, -step % n_y] = lax.ppermute(sent[step], "y", perm)
    right[1, 0, 0] = lax.ppermute(other, "core", cores)
    left[1, 0] = lax.ppermute(left[0, 0], "core", cores)
    for step in range(1, n_y):
        left[1, step] = lax.ppermute(left[0, step], "core", cores)

    for step in range(2, half):
        ring(step, every)
    ring(half, [(0, 0), (1, 1)])

    left_keys = [(flip, step) for flip in range(2) for step in range(n_y)]
    sizes = (rows, slots, n_y, n_lo, n_hi, tb)
    quarter = tb // n_x

    rights = [
        right[key]
        for flip in range(2)
        for key in [(flip, 0, 0)]
        + [(flip, step, chain) for step in range(1, half) for chain in range(2)]
        + [(flip, half, flip)]
    ]
    lefts = [pltpu.with_memory_space_constraint(left[k], pltpu.VMEM) for k in left_keys]
    rights = [pltpu.with_memory_space_constraint(r, pltpu.VMEM) for r in rights]
    early, last = rights[: n_z - 1] + rights[n_z:-1], [rights[n_z - 1], rights[-1]]
    held_shapes = [
        pltpu.VMEM((2 * n_z, payload[0] - TAIL, tb), jnp.bfloat16),
        pltpu.VMEM((2 * n_z * TAIL, tb), jnp.float32),
    ]
    columns, *kept = pl.pallas_call(
        functools.partial(hold_early, rows, len(lefts)),
        out_shape=[pltpu.SMEM((2 * n_y * rows, tb), jnp.int32)] + held_shapes,
        in_specs=[vmem] * (len(lefts) + len(early)),
        out_specs=[pl.BlockSpec(memory_space=pltpu.SMEM)] + [vmem] * 2,
        scratch_shapes=[pltpu.VMEM((2 * n_y * rows, tb), jnp.int32), pltpu.SemaphoreType.DMA],
        compiler_params=limit,
    )(*lefts, *early)
    kept = [pltpu.with_memory_space_constraint(k, pltpu.VMEM) for k in kept]
    operands = [pltpu.with_memory_space_constraint(columns, pltpu.SMEM), *lefts, *last, *kept]
    partial, _, _ = pl.pallas_call(
        functools.partial(products, len(lefts), sizes),
        out_shape=[pltpu.VMEM((2 * n_y, n_x, rows, slots, quarter, tb), jnp.bfloat16)] + held_shapes,
        in_specs=[pl.BlockSpec(memory_space=pltpu.SMEM)] + [vmem] * (len(operands) - 1),
        out_specs=[vmem] * 3,
        input_output_aliases={len(operands) - 2: 1, len(operands) - 1: 2},
        compiler_params=limit,
    )(*operands)

    arrived = lax.all_to_all(
        partial.reshape(2 * n_y * n_x, rows, slots, quarter, tb),
        ("y", "core", "x"),
        split_axis=0,
        concat_axis=0,
        tiled=True,
    )
    arrived = arrived.reshape(n_y, 2, n_x, rows, slots, quarter, tb)
    return pl.pallas_call(
        functools.partial(final_sum, n_y),
        out_shape=jax.ShapeDtypeStruct((rows, groups, slots, quarter, tb), jnp.bfloat16),
        in_specs=[vmem],
        out_specs=vmem,
        compiler_params=limit,
    )(pltpu.with_memory_space_constraint(arrived, pltpu.VMEM))


def solution(mesh):
    fine = Mesh(mesh.devices.reshape(4, 2, 4, 2, 4), ("y", "z_lo", "z_hi", "core", "x"))

    return jax.shard_map(
        on_device,
        mesh=fine,
        in_specs=(P(ROWS_COLS, None, None, None, None), P(ROWS_COLS, None, None)),
        out_specs=P(ROWS_COLS, None, None, "x", None),
        check_vma=False,
    )
```
